256 devices in a mesh: row: 8 (over x, z_hi), col: 32 (over y, z_lo, core).
Axes of the slice: x: 4, y: 4, z: 8 (z_hi: 2, z_lo: 4; z = z_hi * 4 + z_lo), core: 2. Of those that a mesh axis runs over, the one named last changes fastest.
Arguments:
- symmetric: float32 [12288, 12288], P('row', 'col'), may hold values from -24 to 24, as said below
Outputs:
- reduced: float32 [12288, 12288], P('row', 'col')
The draws below stay inside these ranges and needn't reach their ends.
Inputs may be any that keep to these rules, and one draw needn't show every extreme that they name: symmetric equals its transpose.
All inputs are finite; a program needn't handle non-finite values.
Results may differ from the reference program's by a relative error of at most 0.0001.
Values sent between devices are 32-bit elements; how exact they have to be, the bound alone decides.
No kernel may reach another device: no remote copies, remote signals or barrier semaphores. Data moves between devices by JAX's collectives and lax.ppermute only.
A program may use at most 64 MiB of HBM per device.

```python
import math
import jax
import jax.numpy as jnp
from jax import lax

N = 12288
B = 256
PANELS = 1


def draw_symmetric(key, part):
    raw = jax.random.normal(jax.random.fold_in(key, 11), (N, N), jnp.float32)
    result = jnp.clip((raw + raw.T) * 0.70710678, -6.0, 6.0)
    return result


def setup_inputs(seed: int = 0) -> dict:
    keys = jax.random.split(jax.random.key(seed), 2)
    return {
        "symmetric": draw_symmetric(jax.random.fold_in(keys[1], 71), 0),
    }


HIGH = lax.Precision.HIGHEST

def matmul(left_op, right_op):
    return jnp.dot(left_op.astype(jnp.float32), right_op.astype(jnp.float32), precision=HIGH, preferred_element_type=jnp.float32)

def reference(symmetric):
    current = symmetric
    identity = jnp.eye(B, dtype=jnp.float32)
    positions = jnp.arange(N)
    factors = []
    for which in range(PANELS):
        first_col = which * B
        below = first_col + B
        panel_cols = jnp.where((positions >= below)[:, None], current[:, first_col:first_col + B], jnp.float32(0.0))
        gram = matmul(panel_cols.T, panel_cols)
        lower_factor = jnp.linalg.cholesky(gram)
        basis = lax.linalg.triangular_solve(lower_factor, panel_cols, left_side=False, lower=True, transpose_a=True)
        leading = basis[below:below + B]
        reflector = basis.at[below:below + B].add(-identity)
        t_mat = jnp.linalg.solve(identity - leading, identity)
        u_mat = matmul(current, reflector)
        core_sum = matmul(reflector.T, u_mat)
        middle = matmul(matmul(t_mat, core_sum), t_mat.T)
        w_mat = matmul(u_mat, t_mat.T) - 0.5 * matmul(reflector, middle)
        current = current - matmul(reflector, w_mat.T) - matmul(w_mat, reflector.T)
        factors.append(lower_factor.T)
    inverse_root = jnp.float32(1.0 / math.sqrt(N))
    for which in range(PANELS):
        first_col = which * B
        below = first_col + B
        block_vals = jnp.zeros((N - below, B), jnp.float32).at[:B].set(factors[which] * inverse_root)
        current = current.at[below:, first_col:first_col + B].set(block_vals)
        current = current.at[first_col:first_col + B, below:].set(block_vals.T)
    return current
```

```python
import functools
import math

import jax
import jax.numpy as jnp
from jax import lax
from jax.experimental import pallas as pl
from jax.experimental.pallas import tpu as pltpu
from jax.sharding import Mesh
from jax.sharding import PartitionSpec as P

N = 12288
B = 256
ROW = ("x", "zh")
COL = ("y", "zl", "c")
ALL = ROW + COL
SIZES = {"x": 4, "zh": 2, "y": 4, "zl": 4, "c": 2}
HIGHEST = lax.Precision.HIGHEST
INTERPRET = False
STEP = 32


def contract(left_op, right_op, left_dim, right_dim, precision=HIGHEST):
    return lax.dot_general(
        left_op,
        right_op,
        (((left_dim,), (right_dim,)), ((), ())),
        precision=precision,
        preferred_element_type=jnp.float32,
    )


def shifted(value, axis, by):
    size = SIZES[axis]
    return lax.ppermute(value, axis, [(k, (k + by) % size) for k in range(size)])


def gather_over(value, axis, dim=0):
    size = SIZES[axis]
    me = lax.axis_index(axis)
    out = jnp.zeros(value.shape[:dim] + (size,) + value.shape[dim:], value.dtype)
    for by in range(size):
        part = value if by == 0 else shifted(value, axis, by)
        out = lax.dynamic_update_index_in_dim(out, part, (me - by) % size, dim)
    return out


def from_everyone(value, axis):
    size = lax.axis_size(axis)
    return lax.all_to_all(
        jnp.broadcast_to(value[None], (size, *value.shape)), axis, 0, 0, tiled=True
    )


def plane_gather(piece):
    rows, width = piece.shape
    half = width // 2
    left, right = piece[:, :half], piece[:, half:]
    left = gather_over(left, "y")
    right = gather_over(right, "zl")
    left = gather_over(left, "zl", 1)
    right = gather_over(right, "y", 0)
    left = gather_over(left.reshape(16 * rows, half), "c")
    right = gather_over(right.reshape(16 * rows, half), "c")
    return jnp.concatenate(
        [left.reshape(32 * rows, half), right.reshape(32 * rows, half)], axis=1
    )


def row_sum(value):
    return from_everyone(value, ROW).sum(axis=0)


def row_scatter_sum(blocks):
    return lax.all_to_all(blocks, ROW, 0, 0, tiled=True).sum(axis=0)


def row_gather(value):
    return from_everyone(value, ROW).reshape(8 * value.shape[0], value.shape[1])


def plane_place(piece):
    core, rest = divmod(piece, 16)
    return (rest // 4) * 8 + (rest % 4) * 2 + core


TO_PLANE = [
    (r * 32 + j, (j // 4) * 32 + plane_place((j % 4) * 8 + r)) for r in range(8) for j in range(32)
]
TO_ROWS = [(there, here) for here, there in TO_PLANE]


def spread_strip(parts):
    total = None
    for r in range(8):
        moves = [(j, (j // 4) * 32 + plane_place((j % 4) * 8 + r)) for j in range(32)]
        got = lax.ppermute(parts[r], ALL, moves)
        total = got if total is None else total + got
    return total


def mxu(left, right, left_dim=1, right_dim=0):
    return contract(left, right, left_dim, right_dim)


PANEL = 8


def panel_columns(work, at):
    return [
        jnp.broadcast_to(work[:, at + k : at + k + 1], work.shape) for k in range(PANEL)
    ]


def small_chol_inverse(block):
    size = block.shape[0]
    work = jnp.concatenate([block, eye_of(size)], axis=1)
    rows = lax.broadcasted_iota(jnp.int32, (size, 2 * size), 0)
    for at in range(0, size, PANEL):
        columns = panel_columns(work, at)
        for a in range(PANEL):
            k = at + a
            root = lax.rsqrt(columns[a][k : k + 1, :])
            factor = columns[a] * root
            for b in range(a + 1, PANEL):
                columns[b] = columns[b] - factor * factor[at + b : at + b + 1, :]
            line = work[k : k + 1, :] * root
            updated = work - factor * line
            work = jnp.where(rows == k, line, jnp.where(rows > k, updated, work))
    return work[:, size:]


def small_inverse(block):
    size = block.shape[0]
    work = jnp.concatenate([block, eye_of(size)], axis=1)
    rows = lax.broadcasted_iota(jnp.int32, (size, 2 * size), 0)
    for at in range(0, size, PANEL):
        columns = panel_columns(work, at)
        for a in range(PANEL):
            k = at + a
            scale = 1.0 / columns[a][k : k + 1, :]
            factor = jnp.where(rows == k, 1.0, columns[a])
            keep = rows != k
            for b in range(a + 1, PANEL):
                top = columns[b][k : k + 1, :] * scale
                columns[b] = jnp.where(keep, columns[b], 0.0) - jnp.where(
                    keep, factor, -1.0
                ) * top
            line = work[k : k + 1, :] * scale
            work = jnp.where(keep, work - factor * line, line)
    return work[:, size:]


def eye_of(size):
    rows = lax.broadcasted_iota(jnp.int32, (size, size), 0)
    cols = lax.broadcasted_iota(jnp.int32, (size, size), 1)
    return jnp.where(rows == cols, 1.0, 0.0).astype(jnp.float32)


def turned_left(value, by):
    return pltpu.roll(value, (B - by) % B, 1)[:, :STEP]


def chol_kernel(gram_ref, upper_ref, inverse_ref, work):
    lanes = lax.broadcasted_iota(jnp.int32, (STEP, B), 1)
    work[:, :B] = gram_ref[...]
    work[:, B:] = eye_of(B)

    def step(block, carry):
        at = pl.multiple_of(block * STEP, STEP)
        own = work[pl.ds(at, STEP), :]
        inv = small_chol_inverse(turned_left(own[:, :B], at))
        lines = mxu(inv, own)
        work[pl.ds(at, STEP), :] = lines
        ahead = jnp.where(lanes >= at + STEP, lines[:, :B], 0.0)
        work[...] = work[...] - mxu(ahead, lines, 0, 0)
        return carry

    lax.fori_loop(0, B // STEP, step, 0)
    rows = lax.broadcasted_iota(jnp.int32, (B, B), 0)
    cols = lax.broadcasted_iota(jnp.int32, (B, B), 1)
    upper_ref[...] = jnp.where(cols >= rows, work[:, :B], 0.0)
    inverse_ref[...] = jnp.where(cols <= rows, work[:, B:], 0.0)


def t_kernel(lead_ref, inverse_ref, t_ref, work):
    tall = lax.broadcasted_iota(jnp.int32, (B, STEP), 0)
    work[:, :B] = eye_of(B) - mxu(lead_ref[...], inverse_ref[...], 1, 1)
    work[:, B:] = eye_of(B)

    def step(block, carry):
        at = pl.multiple_of(block * STEP, STEP)
        turned = turned_left(work[:, :B], at)
        own = work[pl.ds(at, STEP), :]
        inv = small_inverse(turned_left(own[:, :B], at))
        lines = mxu(inv, own)
        others = jnp.where((tall < at) | (tall >= at + STEP), turned, 0.0)
        work[...] = work[...] - mxu(others, lines)
        work[pl.ds(at, STEP), :] = lines
        return carry

    lax.fori_loop(0, B // STEP, step, 0)
    t_ref[...] = work[:, B:]


def on_squares(kernel, outputs, name, *operands):
    square = jax.ShapeDtypeStruct((B, B), jnp.float32)
    vmem = pl.BlockSpec(memory_space=pltpu.VMEM)
    return pl.pallas_call(
        kernel,
        out_shape=(square,) * outputs,
        in_specs=[vmem] * len(operands),
        out_specs=(vmem,) * outputs,
        scratch_shapes=[pltpu.VMEM((B, 2 * B), jnp.float32)],
        cost_estimate=pl.CostEstimate(
            flops=2_000_000_000, bytes_accessed=4 * B * B * 4, transcendentals=0
        ),
        interpret=INTERPRET,
        name=name,
    )(*operands)


def chol(gram):
    return on_squares(chol_kernel, 2, "chol", gram)


def t_inverse(lead, inverse):
    return on_squares(t_kernel, 1, "tinv", lead, inverse)[0]


def per_device(tile):
    rows_dev, cols_dev = tile.shape
    row_at = lax.axis_index(ROW)
    col_at = lax.axis_index(COL)
    place = (
        lax.axis_index("c") * 16 + lax.axis_index("y") * 4 + lax.axis_index("zl")
    )
    global_cols = col_at * cols_dev + jnp.arange(cols_dev, dtype=jnp.int32)
    global_rows = row_at * rows_dev + jnp.arange(rows_dev, dtype=jnp.int32)
    band = jnp.arange(B, dtype=jnp.int32)
    first = row_at == 0
    zero = jnp.float32(0.0)

    strip = tile[:B, :].T
    strip = jnp.where((global_cols >= B)[:, None], strip, zero)
    panel_part = spread_strip(strip.reshape(8, -1, B))
    panel = plane_gather(panel_part)
    panel_there = lax.ppermute(panel_part, ALL, TO_ROWS)

    gram_own = contract(panel, panel, 0, 0)
    gram_slice = lax.dynamic_slice_in_dim(gram_own, place * 8, 8, 0)
    lead_slice = lax.dynamic_slice_in_dim(panel, B + place * 8, 8, 0)
    lead_slice = jnp.where(first, lead_slice, zero)
    message = row_sum(jnp.concatenate([gram_slice, lead_slice], axis=0))
    message = from_everyone(from_everyone(message, ("y", "zl")), "c")
    message = message.reshape(32, 2, 8, B)
    gram = message[:, 0].reshape(B, B)
    lead = message[:, 1].reshape(B, B)
    upper, inverse = chol(gram)

    unit_i = (global_rows[:, None] - B == band[None, :]).astype(jnp.float32)
    unit_j = (global_cols[:, None] - B == band[None, :]).astype(jnp.float32)
    reflector = contract(panel, inverse, 1, 1) - unit_i
    partial = contract(tile, reflector, 0, 0)
    u_part = row_scatter_sum(partial.reshape(8, -1, B))
    u_mat = plane_gather(lax.ppermute(u_part, ALL, TO_PLANE))
    both_j = row_gather(jnp.concatenate([panel_there, u_part], axis=1))
    reflector_j = contract(both_j[:, :B], inverse, 1, 1) - unit_j
    u_j = both_j[:, B:]
    t_mat = t_inverse(lead, inverse)

    core_own = contract(reflector, u_mat, 0, 0)
    core_slice = lax.dynamic_slice_in_dim(core_own, col_at * 8, 8, 0)
    core_sum = from_everyone(row_sum(core_slice), COL).reshape(B, B)
    middle = contract(contract(t_mat, core_sum, 1, 0), t_mat, 1, 1)

    t_reflector_j = contract(reflector_j, t_mat, 1, 0)
    w_j = contract(u_j, t_mat, 1, 1) - contract(reflector_j, middle, 1, 0)
    current = tile - contract(u_mat, t_reflector_j, 1, 1)
    current = current - contract(reflector, w_j, 1, 1)

    inverse_root = jnp.float32(1.0 / math.sqrt(N))
    r_mat = upper * inverse_root
    old_strip = current[:, :B]
    placed = jnp.zeros((rows_dev, B), jnp.float32).at[B : 2 * B].set(r_mat)
    inside = global_rows[:, None] < 2 * B
    updated = jnp.where(inside, placed, zero)
    updated = jnp.where((col_at == 0) & (global_rows[:, None] >= B), updated, old_strip)
    current = current.at[:, :B].set(updated)
    old_top = current[:B, :]
    mirror = contract(r_mat, unit_j, 0, 1)
    new_top = jnp.where(first & (global_cols >= B)[None, :], mirror, old_top)
    return current.at[:B, :].set(new_top)


def solution(mesh):
    split = Mesh(mesh.devices.reshape(4, 2, 4, 4, 2), ALL)
    return jax.shard_map(
        per_device,
        mesh=split,
        in_specs=(P(ROW, COL),),
        out_specs=P(ROW, COL),
        check_vma=False,
    )
```

```python
import functools
import math

import jax
import jax.numpy as jnp
from jax import lax
from jax.experimental import pallas as pl
from jax.experimental.pallas import tpu as pltpu
from jax.sharding import Mesh
from jax.sharding import PartitionSpec as P

N = 12288
B = 256
ROW = ("x", "zh")
COL = ("y", "zl", "c")
ALL = ROW + COL
SIZES = {"x": 4, "zh": 2, "y": 4, "zl": 4, "c": 2}
HIGHEST = lax.Precision.HIGHEST
INTERPRET = False
STEP = 64


def contract(left_op, right_op, left_dim, right_dim, precision=HIGHEST):
    return lax.dot_general(
        left_op,
        right_op,
        (((left_dim,), (right_dim,)), ((), ())),
        precision=precision,
        preferred_element_type=jnp.float32,
    )


def shifted(value, axis, by):
    size = SIZES[axis]
    return lax.ppermute(value, axis, [(k, (k + by) % size) for k in range(size)])


def gather_over(value, axis, dim=0):
    size = SIZES[axis]
    me = lax.axis_index(axis)
    out = jnp.zeros(value.shape[:dim] + (size,) + value.shape[dim:], value.dtype)
    for by in range(size):
        part = value if by == 0 else shifted(value, axis, by)
        out = lax.dynamic_update_index_in_dim(out, part, (me - by) % size, dim)
    return out


def from_everyone(value, axis):
    size = lax.axis_size(axis)
    return lax.all_to_all(
        jnp.broadcast_to(value[None], (size, *value.shape)), axis, 0, 0, tiled=True
    )


def plane_gather(piece):
    rows, width = piece.shape
    half = width // 2
    left, right = piece[:, :half], piece[:, half:]
    left = gather_over(left, "y")
    right = gather_over(right, "zl")
    left = gather_over(left, "zl", 1)
    right = gather_over(right, "y", 0)
    left = gather_over(left.reshape(16 * rows, half), "c")
    right = gather_over(right.reshape(16 * rows, half), "c")
    return jnp.concatenate(
        [left.reshape(32 * rows, half), right.reshape(32 * rows, half)], axis=1
    )


def row_sum(value):
    return from_everyone(value, ROW).sum(axis=0)


def row_scatter_sum(blocks):
    return lax.all_to_all(blocks, ROW, 0, 0, tiled=True).sum(axis=0)


def row_gather(value):
    return from_everyone(value, ROW).reshape(8 * value.shape[0], value.shape[1])


def plane_place(piece):
    core, rest = divmod(piece, 16)
    return (rest // 4) * 8 + (rest % 4) * 2 + core


TO_PLANE = [
    (r * 32 + j, (j // 4) * 32 + plane_place((j % 4) * 8 + r)) for r in range(8) for j in range(32)
]
TO_ROWS = [(there, here) for here, there in TO_PLANE]


def spread_strip(parts):
    total = None
    for r in range(8):
        moves = [(j, (j // 4) * 32 + plane_place((j % 4) * 8 + r)) for j in range(32)]
        got = lax.ppermute(parts[r], ALL, moves)
        total = got if total is None else total + got
    return total


def mxu(left, right, left_dim=1, right_dim=0):
    return contract(left, right, left_dim, right_dim)


PANEL = 8


def panel_columns(work, at):
    return [
        jnp.broadcast_to(work[:, at + k : at + k + 1], work.shape) for k in range(PANEL)
    ]


def small_chol_inverse(block):
    size = block.shape[0]
    work = jnp.concatenate([block, eye_of(size)], axis=1)
    rows = lax.broadcasted_iota(jnp.int32, (size, 2 * size), 0)
    for at in range(0, size, PANEL):
        columns = panel_columns(work, at)
        for a in range(PANEL):
            k = at + a
            root = lax.rsqrt(columns[a][k : k + 1, :])
            factor = columns[a] * root
            for b in range(a + 1, PANEL):
                columns[b] = columns[b] - factor * factor[at + b : at + b + 1, :]
            line = work[k : k + 1, :] * root
            updated = work - factor * line
            work = jnp.where(rows == k, line, jnp.where(rows > k, updated, work))
    return work[:, size:]


def small_inverse(block):
    size = block.shape[0]
    work = jnp.concatenate([block, eye_of(size)], axis=1)
    rows = lax.broadcasted_iota(jnp.int32, (size, 2 * size), 0)
    for at in range(0, size, PANEL):
        columns = panel_columns(work, at)
        for a in range(PANEL):
            k = at + a
            scale = 1.0 / columns[a][k : k + 1, :]
            factor = jnp.where(rows == k, 1.0, columns[a])
            keep = rows != k
            for b in range(a + 1, PANEL):
                top = columns[b][k : k + 1, :] * scale
                columns[b] = jnp.where(keep, columns[b], 0.0) - jnp.where(
                    keep, factor, -1.0
                ) * top
            line = work[k : k + 1, :] * scale
            work = jnp.where(keep, work - factor * line, line)
    return work[:, size:]


def eye_of(size):
    rows = lax.broadcasted_iota(jnp.int32, (size, size), 0)
    cols = lax.broadcasted_iota(jnp.int32, (size, size), 1)
    return jnp.where(rows == cols, 1.0, 0.0).astype(jnp.float32)


def turned_left(value, by):
    return pltpu.roll(value, (B - by) % B, 1)[:, :STEP]


def chol_kernel(gram_ref, upper_ref, inverse_ref, work):
    lanes = lax.broadcasted_iota(jnp.int32, (STEP, B), 1)
    work[:, :B] = gram_ref[...]
    work[:, B:] = eye_of(B)

    def step(block, carry):
        at = pl.multiple_of(block * STEP, STEP)
        own = work[pl.ds(at, STEP), :]
        inv = small_chol_inverse(turned_left(own[:, :B], at))
        lines = mxu(inv, own)
        work[pl.ds(at, STEP), :] = lines
        ahead = jnp.where(lanes >= at + STEP, lines[:, :B], 0.0)
        work[...] = work[...] - mxu(ahead, lines, 0, 0)
        return carry

    lax.fori_loop(0, B // STEP, step, 0)
    rows = lax.broadcasted_iota(jnp.int32, (B, B), 0)
    cols = lax.broadcasted_iota(jnp.int32, (B, B), 1)
    upper_ref[...] = jnp.where(cols >= rows, work[:, :B], 0.0)
    inverse_ref[...] = jnp.where(cols <= rows, work[:, B:], 0.0)


def t_kernel(lead_ref, inverse_ref, t_ref, work):
    tall = lax.broadcasted_iota(jnp.int32, (B, STEP), 0)
    work[:, :B] = eye_of(B) - mxu(lead_ref[...], inverse_ref[...], 1, 1)
    work[:, B:] = eye_of(B)

    def step(block, carry):
        at = pl.multiple_of(block * STEP, STEP)
        turned = turned_left(work[:, :B], at)
        own = work[pl.ds(at, STEP), :]
        inv = small_inverse(turned_left(own[:, :B], at))
        lines = mxu(inv, own)
        others = jnp.where((tall < at) | (tall >= at + STEP), turned, 0.0)
        work[...] = work[...] - mxu(others, lines)
        work[pl.ds(at, STEP), :] = lines
        return carry

    lax.fori_loop(0, B // STEP, step, 0)
    t_ref[...] = work[:, B:]


def on_squares(kernel, outputs, name, *operands):
    square = jax.ShapeDtypeStruct((B, B), jnp.float32)
    vmem = pl.BlockSpec(memory_space=pltpu.VMEM)
    return pl.pallas_call(
        kernel,
        out_shape=(square,) * outputs,
        in_specs=[vmem] * len(operands),
        out_specs=(vmem,) * outputs,
        scratch_shapes=[pltpu.VMEM((B, 2 * B), jnp.float32)],
        cost_estimate=pl.CostEstimate(
            flops=2_000_000_000, bytes_accessed=4 * B * B * 4, transcendentals=0
        ),
        interpret=INTERPRET,
        name=name,
    )(*operands)


def chol(gram):
    return on_squares(chol_kernel, 2, "chol", gram)


def t_inverse(lead, inverse):
    return on_squares(t_kernel, 1, "tinv", lead, inverse)[0]


def update_kernel(at_ref, tile_ref, v_ref, u_ref, w_ref, tv_ref, r_ref, rt_ref, out_ref, factors):
    row_at, col_at = at_ref[0], at_ref[1]
    step = pl.program_id(0)

    @pl.when(step == 0)
    def _():
        for k, ref in enumerate((w_ref, tv_ref)):
            high = ref[...].astype(jnp.bfloat16)
            factors[2 * k] = high
            factors[2 * k + 1] = (ref[...] - high.astype(jnp.float32)).astype(jnp.bfloat16)

    def times(value, high, low):
        value_high = value.astype(jnp.bfloat16)
        value_low = (value - value_high.astype(jnp.float32)).astype(jnp.bfloat16)

        def dot(left, right):
            return lax.dot_general(
                left, right, (((1,), (1,)), ((), ())), preferred_element_type=jnp.float32
            )

        return dot(value_high, high) + (dot(value_high, low) + dot(value_low, high))

    out_ref[...] = tile_ref[...] - (
        times(v_ref[...], factors[0], factors[1]) + times(u_ref[...], factors[2], factors[3])
    )
    top = (row_at == 0) & (step == 0)

    @pl.when((col_at == 0) & jnp.logical_not(top))
    def _():
        out_ref[:, :B] = jnp.zeros((B, B), jnp.float32)

    @pl.when((col_at == 0) & (row_at == 0) & (step == 1))
    def _():
        out_ref[:, :B] = r_ref[...]

    @pl.when(top & (col_at == 0))
    def _():
        out_ref[:, B:] = rt_ref[:, : B // 2]

    @pl.when(top & (col_at == 1))
    def _():
        out_ref[:, : B // 2] = rt_ref[:, B // 2 :]
        out_ref[:, B // 2 :] = jnp.zeros((B, B), jnp.float32)

    @pl.when(top & (col_at >= 2))
    def _():
        out_ref[...] = jnp.zeros(out_ref.shape, jnp.float32)


def updated(at, tile, reflector, u_mat, w_j, t_reflector_j, upper):
    rows_dev, cols_dev = tile.shape

    def whole(shape):
        return pl.BlockSpec(shape, lambda k, at: (0, 0))

    def lines(width):
        return pl.BlockSpec((B, width), lambda k, at: (k, 0))

    return pl.pallas_call(
        update_kernel,
        out_shape=jax.ShapeDtypeStruct(tile.shape, jnp.float32),
        grid_spec=pltpu.PrefetchScalarGridSpec(
            num_scalar_prefetch=1,
            grid=(rows_dev // B,),
            in_specs=[
                lines(cols_dev),
                lines(B),
                lines(B),
                whole((cols_dev, B)),
                whole((cols_dev, B)),
                whole((B, B)),
                whole((B, B)),
            ],
            out_specs=lines(cols_dev),
            scratch_shapes=[pltpu.VMEM((4, cols_dev, B), jnp.bfloat16)],
        ),
        cost_estimate=pl.CostEstimate(
            flops=6 * 2 * rows_dev * cols_dev * B,
            bytes_accessed=4 * rows_dev * (2 * cols_dev + 2 * B),
            transcendentals=0,
        ),
        interpret=INTERPRET,
        name="update",
    )(at, tile, reflector, u_mat, w_j, t_reflector_j, upper, upper.T)


def per_device(tile):
    rows_dev, cols_dev = tile.shape
    row_at = lax.axis_index(ROW)
    col_at = lax.axis_index(COL)
    global_cols = col_at * cols_dev + jnp.arange(cols_dev, dtype=jnp.int32)
    global_rows = row_at * rows_dev + jnp.arange(rows_dev, dtype=jnp.int32)
    band = jnp.arange(B, dtype=jnp.int32)
    zero = jnp.float32(0.0)

    top = jnp.where((global_cols >= B)[None, :], tile[:B, :], zero)
    strip = top.T

    gram_part = contract(top, top, 1, 1).reshape(32, 8, B)
    lead_part = jnp.concatenate(
        [
            jnp.where(col_at == 0, strip[B:], zero),
            jnp.where(col_at == 1, strip[: B // 2], zero),
        ],
        axis=0,
    ).reshape(32, 8, B)
    message = jnp.concatenate([gram_part, lead_part], axis=1)
    message = lax.all_to_all(message, COL, 0, 0, tiled=True).sum(axis=0)
    message = from_everyone(from_everyone(message, ROW)[0], COL)
    gram = message[:, :8].reshape(B, B)
    lead = message[:, 8:].reshape(B, B)
    upper, inverse = chol(gram)
    t_mat = t_inverse(lead, inverse)

    panel_part = spread_strip(strip.reshape(8, -1, B))
    panel = plane_gather(panel_part)
    panel_there = lax.ppermute(panel_part, ALL, TO_ROWS)

    unit_i = (global_rows[:, None] - B == band[None, :]).astype(jnp.float32)
    unit_j = (global_cols[:, None] - B == band[None, :]).astype(jnp.float32)
    reflector = contract(panel, inverse, 1, 1) - unit_i
    partial = contract(tile, reflector, 0, 0, lax.Precision.HIGH)
    u_part = row_scatter_sum(partial.reshape(8, -1, B))
    u_mat = plane_gather(lax.ppermute(u_part, ALL, TO_PLANE))
    both_j = row_gather(jnp.concatenate([panel_there, u_part], axis=1))
    reflector_j = contract(both_j[:, :B], inverse, 1, 1) - unit_j
    u_j = both_j[:, B:]

    core_part = contract(reflector_j, u_j, 0, 0).reshape(32, 8, B)
    core_part = lax.all_to_all(core_part, COL, 0, 0, tiled=True).sum(axis=0)
    core_sum = from_everyone(core_part, COL).reshape(B, B)
    middle = contract(contract(t_mat, core_sum, 1, 0), t_mat, 1, 1)

    t_reflector_j = contract(reflector_j, t_mat, 1, 0)
    w_j = contract(u_j, t_mat, 1, 1) - contract(reflector_j, middle, 1, 0)
    return updated(
        jnp.stack([row_at, col_at]).astype(jnp.int32),
        tile,
        reflector,
        u_mat,
        w_j,
        t_reflector_j,
        upper * jnp.float32(1.0 / math.sqrt(N)),
    )


def solution(mesh):
    split = Mesh(mesh.devices.reshape(4, 2, 4, 4, 2), ALL)
    return jax.shard_map(
        per_device,
        mesh=split,
        in_specs=(P(ROW, COL),),
        out_specs=P(ROW, COL),
        check_vma=False,
    )
```

```python
import functools
import math

import jax
import jax.numpy as jnp
from jax import lax
from jax.experimental import pallas as pl
from jax.experimental.pallas import tpu as pltpu
from jax.sharding import Mesh
from jax.sharding import PartitionSpec as P

N = 12288
B = 256
ROW = ("x", "zh")
COL = ("y", "zl", "c")
ALL = ROW + COL
SIZES = {"x": 4, "zh": 2, "y": 4, "zl": 4, "c": 2}
HIGHEST = lax.Precision.HIGHEST
INTERPRET = False
STEP = 64


def contract(left_op, right_op, left_dim, right_dim, precision=HIGHEST):
    return lax.dot_general(
        left_op,
        right_op,
        (((left_dim,), (right_dim,)), ((), ())),
        precision=precision,
        preferred_element_type=jnp.float32,
    )


def shifted(value, axis, by):
    size = SIZES[axis]
    return lax.ppermute(value, axis, [(k, (k + by) % size) for k in range(size)])


def gather_over(value, axis, dim=0):
    size = SIZES[axis]
    me = lax.axis_index(axis)
    out = jnp.zeros(value.shape[:dim] + (size,) + value.shape[dim:], value.dtype)
    for by in range(size):
        part = value if by == 0 else shifted(value, axis, by)
        out = lax.dynamic_update_index_in_dim(out, part, (me - by) % size, dim)
    return out


def from_everyone(value, axis):
    size = lax.axis_size(axis)
    return lax.all_to_all(
        jnp.broadcast_to(value[None], (size, *value.shape)), axis, 0, 0, tiled=True
    )


def plane_gather(piece, tied=None):
    rows, width = piece.shape
    half = width // 2
    left, right = piece[:, :half], piece[:, half:]
    left = gather_over(left, "y")
    right = gather_over(right, "zl")
    if tied is not None:
        left, right, tied = lax.optimization_barrier((left, right, tied))
    left = gather_over(left, "zl", 1)
    right = gather_over(right, "y", 0)
    left = gather_over(left.reshape(16 * rows, half), "c")
    right = gather_over(right.reshape(16 * rows, half), "c")
    whole = jnp.concatenate(
        [left.reshape(32 * rows, half), right.reshape(32 * rows, half)], axis=1
    )
    return whole if tied is None else (whole, tied)


def row_sum(value):
    return from_everyone(value, ROW).sum(axis=0)


def row_scatter_sum(blocks):
    return lax.all_to_all(blocks, ROW, 0, 0, tiled=True).sum(axis=0)


def row_gather(value):
    return from_everyone(value, ROW).reshape(8 * value.shape[0], value.shape[1])


def plane_place(piece):
    core, rest = divmod(piece, 16)
    return (rest // 4) * 8 + (rest % 4) * 2 + core


TO_PLANE = [
    (r * 32 + j, (j // 4) * 32 + plane_place((j % 4) * 8 + r)) for r in range(8) for j in range(32)
]
TO_ROWS = [(there, here) for here, there in TO_PLANE]


def spread_strip(parts):
    total = None
    for r in range(8):
        moves = [(j, (j // 4) * 32 + plane_place((j % 4) * 8 + r)) for j in range(32)]
        got = lax.ppermute(parts[r], ALL, moves)
        total = got if total is None else total + got
    return total


def mxu(left, right, left_dim=1, right_dim=0):
    return contract(left, right, left_dim, right_dim)


PANEL = 8


def panel_columns(work, at):
    return [
        jnp.broadcast_to(work[:, at + k : at + k + 1], work.shape) for k in range(PANEL)
    ]


def small_chol_inverse(block):
    size = block.shape[0]
    work = jnp.concatenate([block, eye_of(size)], axis=1)
    rows = lax.broadcasted_iota(jnp.int32, (size, 2 * size), 0)
    for at in range(0, size, PANEL):
        columns = panel_columns(work, at)
        for a in range(PANEL):
            k = at + a
            root = lax.rsqrt(columns[a][k : k + 1, :])
            factor = columns[a] * root
            for b in range(a + 1, PANEL):
                columns[b] = columns[b] - factor * factor[at + b : at + b + 1, :]
            line = work[k : k + 1, :] * root
            updated = work - factor * line
            work = jnp.where(rows == k, line, jnp.where(rows > k, updated, work))
    return work[:, size:]


def small_inverse(block):
    size = block.shape[0]
    work = jnp.concatenate([block, eye_of(size)], axis=1)
    rows = lax.broadcasted_iota(jnp.int32, (size, 2 * size), 0)
    for at in range(0, size, PANEL):
        columns = panel_columns(work, at)
        for a in range(PANEL):
            k = at + a
            scale = 1.0 / columns[a][k : k + 1, :]
            factor = jnp.where(rows == k, 1.0, columns[a])
            keep = rows != k
            for b in range(a + 1, PANEL):
                top = columns[b][k : k + 1, :] * scale
                columns[b] = jnp.where(keep, columns[b], 0.0) - jnp.where(
                    keep, factor, -1.0
                ) * top
            line = work[k : k + 1, :] * scale
            work = jnp.where(keep, work - factor * line, line)
    return work[:, size:]


def eye_of(size):
    rows = lax.broadcasted_iota(jnp.int32, (size, size), 0)
    cols = lax.broadcasted_iota(jnp.int32, (size, size), 1)
    return jnp.where(rows == cols, 1.0, 0.0).astype(jnp.float32)


def turned_left(value, by):
    return pltpu.roll(value, (B - by) % B, 1)[:, :STEP]


def chol_kernel(gram_ref, upper_ref, inverse_ref, work):
    lanes = lax.broadcasted_iota(jnp.int32, (STEP, B), 1)
    work[:, :B] = gram_ref[...]
    work[:, B:] = eye_of(B)

    def step(block, carry):
        at = pl.multiple_of(block * STEP, STEP)
        own = work[pl.ds(at, STEP), :]
        inv = small_chol_inverse(turned_left(own[:, :B], at))
        lines = mxu(inv, own)
        work[pl.ds(at, STEP), :] = lines
        ahead = jnp.where(lanes >= at + STEP, lines[:, :B], 0.0)
        work[...] = work[...] - mxu(ahead, lines, 0, 0)
        return carry

    lax.fori_loop(0, B // STEP, step, 0)
    rows = lax.broadcasted_iota(jnp.int32, (B, B), 0)
    cols = lax.broadcasted_iota(jnp.int32, (B, B), 1)
    upper_ref[...] = jnp.where(cols >= rows, work[:, :B], 0.0)
    inverse_ref[...] = jnp.where(cols <= rows, work[:, B:], 0.0)


def t_kernel(lead_ref, inverse_ref, t_ref, work):
    tall = lax.broadcasted_iota(jnp.int32, (B, STEP), 0)
    work[:, :B] = eye_of(B) - mxu(lead_ref[...], inverse_ref[...], 1, 1)
    work[:, B:] = eye_of(B)

    def step(block, carry):
        at = pl.multiple_of(block * STEP, STEP)
        turned = turned_left(work[:, :B], at)
        own = work[pl.ds(at, STEP), :]
        inv = small_inverse(turned_left(own[:, :B], at))
        lines = mxu(inv, own)
        others = jnp.where((tall < at) | (tall >= at + STEP), turned, 0.0)
        work[...] = work[...] - mxu(others, lines)
        work[pl.ds(at, STEP), :] = lines
        return carry

    lax.fori_loop(0, B // STEP, step, 0)
    t_ref[...] = work[:, B:]


def on_squares(kernel, outputs, name, *operands):
    square = jax.ShapeDtypeStruct((B, B), jnp.float32)
    vmem = pl.BlockSpec(memory_space=pltpu.VMEM)
    return pl.pallas_call(
        kernel,
        out_shape=(square,) * outputs,
        in_specs=[vmem] * len(operands),
        out_specs=(vmem,) * outputs,
        scratch_shapes=[pltpu.VMEM((B, 2 * B), jnp.float32)],
        cost_estimate=pl.CostEstimate(
            flops=2_000_000_000, bytes_accessed=4 * B * B * 4, transcendentals=0
        ),
        interpret=INTERPRET,
        name=name,
    )(*operands)


def chol(gram):
    return on_squares(chol_kernel, 2, "chol", gram)


def t_inverse(lead, inverse):
    return on_squares(t_kernel, 1, "tinv", lead, inverse)[0]


def dot(left, right, left_dim, right_dim):
    return lax.dot_general(
        left, right, (((left_dim,), (right_dim,)), ((), ())), preferred_element_type=jnp.float32
    )


def parts_of(value):
    high = value.astype(jnp.bfloat16)
    return high, (value - high.astype(jnp.float32)).astype(jnp.bfloat16)


def split_dot(left, right, left_dim, right_dim):
    left_high, left_low = left
    right_high, right_low = right
    return dot(left_high, right_high, left_dim, right_dim) + (
        dot(left_high, right_low, left_dim, right_dim)
        + dot(left_low, right_high, left_dim, right_dim)
    )


def gram_kernel(panel_ref, out_ref):
    @pl.when(pl.program_id(0) == 0)
    def _():
        out_ref[...] = jnp.zeros(out_ref.shape, jnp.float32)

    out_ref[...] += mxu(panel_ref[...], panel_ref[...], 0, 0)


def gram_of(panel):
    return pl.pallas_call(
        gram_kernel,
        out_shape=jax.ShapeDtypeStruct((B, B), jnp.float32),
        grid=(panel.shape[0] // B,),
        in_specs=[pl.BlockSpec((B, B), lambda k: (k, 0))],
        out_specs=pl.BlockSpec((B, B), lambda k: (0, 0)),
        cost_estimate=pl.CostEstimate(
            flops=12 * panel.shape[0] * B * B, bytes_accessed=4 * panel.size, transcendentals=0
        ),
        interpret=INTERPRET,
        name="gram",
    )(panel)


def reflect_kernel(at_ref, tile_ref, panel_ref, inverse_ref, v_ref, out_ref):
    step = pl.program_id(0)
    v_ref[...] = mxu(panel_ref[...], inverse_ref[...], 1, 1)

    @pl.when((step == 1) & (at_ref[0] == 0))
    def _():
        v_ref[...] = v_ref[...] - eye_of(B)

    @pl.when(step == 0)
    def _():
        out_ref[...] = jnp.zeros(out_ref.shape, jnp.float32)

    out_ref[...] += split_dot(parts_of(tile_ref[...]), parts_of(v_ref[...]), 0, 0)


def reflected(at, tile, panel, inverse):
    rows_dev, cols_dev = tile.shape
    return pl.pallas_call(
        reflect_kernel,
        out_shape=(
            jax.ShapeDtypeStruct((rows_dev, B), jnp.float32),
            jax.ShapeDtypeStruct((cols_dev, B), jnp.float32),
        ),
        grid_spec=pltpu.PrefetchScalarGridSpec(
            num_scalar_prefetch=1,
            grid=(rows_dev // B,),
            in_specs=[
                pl.BlockSpec((B, cols_dev), lambda k, at: (k, 0)),
                pl.BlockSpec((B, B), lambda k, at: (k, 0)),
                pl.BlockSpec((B, B), lambda k, at: (0, 0)),
            ],
            out_specs=(
                pl.BlockSpec((B, B), lambda k, at: (k, 0)),
                pl.BlockSpec((cols_dev, B), lambda k, at: (0, 0)),
            ),
        ),
        cost_estimate=pl.CostEstimate(
            flops=6 * rows_dev * (cols_dev + 2 * B) * B,
            bytes_accessed=4 * rows_dev * (cols_dev + 2 * B),
            transcendentals=0,
        ),
        interpret=INTERPRET,
        name="reflect",
    )(at, tile, panel, inverse)


def update_kernel(at_ref, tile_ref, v_ref, u_ref, w_ref, tv_ref, r_ref, rt_ref, out_ref, factors):
    row_at, col_at = at_ref[0], at_ref[1]
    step = pl.program_id(0)

    @pl.when(step == 0)
    def _():
        factors[0], factors[1] = parts_of(w_ref[...])
        factors[2], factors[3] = parts_of(tv_ref[...])

    out_ref[...] = tile_ref[...] - (
        split_dot(parts_of(v_ref[...]), (factors[0], factors[1]), 1, 0)
        + split_dot(parts_of(u_ref[...]), (factors[2], factors[3]), 1, 0)
    )
    top = (row_at == 0) & (step == 0)

    @pl.when((col_at == 0) & jnp.logical_not(top))
    def _():
        out_ref[:, :B] = jnp.zeros((B, B), jnp.float32)

    @pl.when((col_at == 0) & (row_at == 0) & (step == 1))
    def _():
        out_ref[:, :B] = r_ref[...]

    @pl.when(top & (col_at == 0))
    def _():
        out_ref[:, B:] = rt_ref[:, : B // 2]

    @pl.when(top & (col_at == 1))
    def _():
        out_ref[:, : B // 2] = rt_ref[:, B // 2 :]
        out_ref[:, B // 2 :] = jnp.zeros((B, B), jnp.float32)

    @pl.when(top & (col_at >= 2))
    def _():
        out_ref[...] = jnp.zeros(out_ref.shape, jnp.float32)


def updated(at, tile, reflector, u_mat, w_trans, t_reflector_trans, upper):
    rows_dev, cols_dev = tile.shape

    def whole(shape):
        return pl.BlockSpec(shape, lambda k, at: (0, 0))

    def lines(width):
        return pl.BlockSpec((B, width), lambda k, at: (k, 0))

    return pl.pallas_call(
        update_kernel,
        out_shape=jax.ShapeDtypeStruct(tile.shape, jnp.float32),
        grid_spec=pltpu.PrefetchScalarGridSpec(
            num_scalar_prefetch=1,
            grid=(rows_dev // B,),
            in_specs=[
                lines(cols_dev),
                lines(B),
                lines(B),
                whole((B, cols_dev)),
                whole((B, cols_dev)),
                whole((B, B)),
                whole((B, B)),
            ],
            out_specs=lines(cols_dev),
            scratch_shapes=[pltpu.VMEM((4, B, cols_dev), jnp.bfloat16)],
        ),
        cost_estimate=pl.CostEstimate(
            flops=6 * 2 * rows_dev * cols_dev * B,
            bytes_accessed=4 * rows_dev * (2 * cols_dev + 2 * B),
            transcendentals=0,
        ),
        interpret=INTERPRET,
        name="update",
    )(at, tile, reflector, u_mat, w_trans, t_reflector_trans, upper, upper.T)


def per_device(tile):
    rows_dev, cols_dev = tile.shape
    row_at = lax.axis_index(ROW)
    col_at = lax.axis_index(COL)
    global_cols = col_at * cols_dev + jnp.arange(cols_dev, dtype=jnp.int32)
    band = jnp.arange(B, dtype=jnp.int32)
    zero = jnp.float32(0.0)

    place = (
        lax.axis_index("c") * 16 + lax.axis_index("y") * 4 + lax.axis_index("zl")
    )
    at = jnp.stack([row_at, col_at]).astype(jnp.int32)

    strip = jnp.where((global_cols >= B)[:, None], tile[:B, :].T, zero)
    panel_part = spread_strip(strip.reshape(8, -1, B))
    panel = plane_gather(panel_part)
    panel_there = lax.ppermute(panel_part, ALL, TO_ROWS)

    gram_slice = lax.dynamic_slice_in_dim(gram_of(panel), place * 8, 8, 0)
    lead_slice = lax.dynamic_slice_in_dim(panel, B + place * 8, 8, 0)
    lead_slice = jnp.where(row_at == 0, lead_slice, zero)
    message = row_sum(jnp.concatenate([gram_slice, lead_slice], axis=0))
    message = from_everyone(from_everyone(message, ("y", "zl")), "c")
    message = message.reshape(32, 2, 8, B)
    gram = message[:, 0].reshape(B, B)
    lead = message[:, 1].reshape(B, B)
    upper, inverse = chol(gram)
    t_mat = t_inverse(lead, inverse)

    unit_j = (global_cols[:, None] - B == band[None, :]).astype(jnp.float32)
    reflector, partial = reflected(at, tile, panel, inverse)
    u_part = row_scatter_sum(partial.reshape(8, -1, B))
    u_there = lax.ppermute(u_part, ALL, TO_PLANE)
    both_j = row_gather(jnp.concatenate([panel_there, u_part], axis=1))
    reflector_j = contract(both_j[:, :B], inverse, 1, 1) - unit_j
    u_j = both_j[:, B:]

    core_part = contract(reflector_j, u_j, 0, 0).reshape(32, 8, B)
    u_there, core_part = lax.optimization_barrier((u_there, core_part))
    core_part = lax.all_to_all(core_part, COL, 0, 0, tiled=True).sum(axis=0)
    u_mat, core_part = plane_gather(u_there, core_part)
    core_sum = from_everyone(core_part, COL).reshape(B, B)
    middle = contract(contract(t_mat, core_sum, 1, 0), t_mat, 1, 1)

    t_reflector_trans = contract(t_mat, reflector_j, 0, 1)
    w_trans = contract(t_mat, u_j, 1, 1) - contract(middle, reflector_j, 1, 1)
    return updated(
        at,
        tile,
        reflector,
        u_mat,
        w_trans,
        t_reflector_trans,
        upper * jnp.float32(1.0 / math.sqrt(N)),
    )


def solution(mesh):
    split = Mesh(mesh.devices.reshape(4, 2, 4, 4, 2), ALL)
    return jax.shard_map(
        per_device,
        mesh=split,
        in_specs=(P(ROW, COL),),
        out_specs=P(ROW, COL),
        check_vma=False,
    )
```

```python
import math

import jax
import jax.numpy as jnp
from jax import lax
from jax.experimental import pallas as pl
from jax.experimental.pallas import tpu as pltpu
from jax.sharding import Mesh
from jax.sharding import PartitionSpec as P


N = 12288
B = 256
ROW = ("x", "zh")
COL = ("y", "zl", "c")
ALL = ROW + COL
SIZES = {"x": 4, "zh": 2, "y": 4, "zl": 4, "c": 2}
HIGHEST = lax.Precision.HIGHEST
INTERPRET = False
STEP = 64


def contract(left_op, right_op, left_dim, right_dim, precision=HIGHEST):
    return lax.dot_general(
        left_op,
        right_op,
        (((left_dim,), (right_dim,)), ((), ())),
        precision=precision,
        preferred_element_type=jnp.float32,
    )


def shifted(value, axis, by):
    size = SIZES[axis]
    return lax.ppermute(value, axis, [(k, (k + by) % size) for k in range(size)])


def gather_over(value, axis, dim=0):
    size = SIZES[axis]
    me = lax.axis_index(axis)
    out = jnp.zeros(value.shape[:dim] + (size,) + value.shape[dim:], value.dtype)
    for by in range(size):
        part = value if by == 0 else shifted(value, axis, by)
        out = lax.dynamic_update_index_in_dim(out, part, (me - by) % size, dim)
    return out


def from_everyone(value, axis):
    size = lax.axis_size(axis)
    return lax.all_to_all(
        jnp.broadcast_to(value[None], (size, *value.shape)), axis, 0, 0, tiled=True
    )


def plane_gather(piece, tied=None):
    rows, width = piece.shape
    half = width // 2
    left = gather_over(piece[:, :half], "y")
    right = gather_over(piece[:, half:], "zl")
    if tied is not None:
        left, right, tied = lax.optimization_barrier((left, right, tied))
    left = gather_over(left, "zl", 1)
    right = gather_over(right, "y", 0)
    left = gather_over(left.reshape(16 * rows, half), "c")
    right = gather_over(right.reshape(16 * rows, half), "c")
    left, right = left.reshape(32 * rows, half), right.reshape(32 * rows, half)
    return (left, right) if tied is None else (left, right, tied)


def row_gather(value):
    return from_everyone(value, ROW).reshape(8 * value.shape[0], value.shape[1])


def plane_place(piece):
    core, rest = divmod(piece, 16)
    return (rest // 4) * 8 + (rest % 4) * 2 + core


TO_PLANE = [
    (r * 32 + j, (j // 4) * 32 + plane_place((j % 4) * 8 + r)) for r in range(8) for j in range(32)
]


def spread_strip(parts):
    total = None
    for r in range(8):
        moves = [(j, (j // 4) * 32 + plane_place((j % 4) * 8 + r)) for j in range(32)]
        got = lax.ppermute(parts[r], ALL, moves)
        total = got if total is None else total + got
    return total


def mxu(left, right, left_dim=1, right_dim=0):
    return contract(left, right, left_dim, right_dim)


PANEL = 8


def panel_columns(work, at):
    return [
        jnp.broadcast_to(work[:, at + k : at + k + 1], work.shape) for k in range(PANEL)
    ]


def small_chol_inverse(block):
    size = block.shape[0]
    work = jnp.concatenate([block, eye_of(size)], axis=1)
    rows = lax.broadcasted_iota(jnp.int32, (size, 2 * size), 0)
    for at in range(0, size, PANEL):
        columns = panel_columns(work, at)
        for a in range(PANEL):
            k = at + a
            root = lax.rsqrt(columns[a][k : k + 1, :])
            factor = columns[a] * root
            for b in range(a + 1, PANEL):
                columns[b] = columns[b] - factor * factor[at + b : at + b + 1, :]
            line = work[k : k + 1, :] * root
            updated = work - factor * line
            work = jnp.where(rows == k, line, jnp.where(rows > k, updated, work))
    return work[:, size:]


def small_inverse(block):
    size = block.shape[0]
    work = jnp.concatenate([block, eye_of(size)], axis=1)
    rows = lax.broadcasted_iota(jnp.int32, (size, 2 * size), 0)
    for at in range(0, size, PANEL):
        columns = panel_columns(work, at)
        for a in range(PANEL):
            k = at + a
            scale = 1.0 / columns[a][k : k + 1, :]
            factor = jnp.where(rows == k, 1.0, columns[a])
            keep = rows != k
            for b in range(a + 1, PANEL):
                top = columns[b][k : k + 1, :] * scale
                columns[b] = jnp.where(keep, columns[b], 0.0) - jnp.where(
                    keep, factor, -1.0
                ) * top
            line = work[k : k + 1, :] * scale
            work = jnp.where(keep, work - factor * line, line)
    return work[:, size:]


def eye_of(size):
    rows = lax.broadcasted_iota(jnp.int32, (size, size), 0)
    cols = lax.broadcasted_iota(jnp.int32, (size, size), 1)
    return jnp.where(rows == cols, 1.0, 0.0).astype(jnp.float32)


def turned_left(value, by):
    return pltpu.roll(value, (B - by) % B, 1)[:, :STEP]


def chol_kernel(gram_ref, upper_ref, inverse_ref, work):
    lanes = lax.broadcasted_iota(jnp.int32, (STEP, B), 1)
    work[:, :B] = gram_ref[...]
    work[:, B:] = eye_of(B)

    def step(block, carry):
        at = pl.multiple_of(block * STEP, STEP)
        own = work[pl.ds(at, STEP), :]
        inv = small_chol_inverse(turned_left(own[:, :B], at))
        lines = mxu(inv, own)
        work[pl.ds(at, STEP), :] = lines
        ahead = jnp.where(lanes >= at + STEP, lines[:, :B], 0.0)
        work[...] = work[...] - mxu(ahead, lines, 0, 0)
        return carry

    lax.fori_loop(0, B // STEP, step, 0)
    rows = lax.broadcasted_iota(jnp.int32, (B, B), 0)
    cols = lax.broadcasted_iota(jnp.int32, (B, B), 1)
    upper_ref[...] = jnp.where(cols >= rows, work[:, :B], 0.0)
    inverse_ref[...] = jnp.where(cols <= rows, work[:, B:], 0.0)


def t_kernel(lead_ref, inverse_ref, t_ref, work):
    tall = lax.broadcasted_iota(jnp.int32, (B, STEP), 0)
    work[:, :B] = eye_of(B) - mxu(lead_ref[...], inverse_ref[...], 1, 1)
    work[:, B:] = eye_of(B)

    def step(block, carry):
        at = pl.multiple_of(block * STEP, STEP)
        turned = turned_left(work[:, :B], at)
        own = work[pl.ds(at, STEP), :]
        inv = small_inverse(turned_left(own[:, :B], at))
        lines = mxu(inv, own)
        others = jnp.where((tall < at) | (tall >= at + STEP), turned, 0.0)
        work[...] = work[...] - mxu(others, lines)
        work[pl.ds(at, STEP), :] = lines
        return carry

    lax.fori_loop(0, B // STEP, step, 0)
    t_ref[...] = work[:, B:]


def on_squares(kernel, outputs, *operands):
    square = jax.ShapeDtypeStruct((B, B), jnp.float32)
    vmem = pl.BlockSpec(memory_space=pltpu.VMEM)
    return pl.pallas_call(
        kernel,
        out_shape=(square,) * outputs,
        in_specs=[vmem] * len(operands),
        out_specs=(vmem,) * outputs,
        scratch_shapes=[pltpu.VMEM((B, 2 * B), jnp.float32)],
        cost_estimate=pl.CostEstimate(
            flops=2_000_000_000, bytes_accessed=4 * B * B * 4, transcendentals=0
        ),
        interpret=INTERPRET,
    )(*operands)


def chol(gram):
    return on_squares(chol_kernel, 2, gram)


def t_inverse(lead, inverse):
    return on_squares(t_kernel, 1, lead, inverse)[0]


def dot(left, right, left_dim, right_dim):
    return lax.dot_general(
        left, right, (((left_dim,), (right_dim,)), ((), ())), preferred_element_type=jnp.float32
    )


def bf16_parts(value, count):
    parts = []
    for _ in range(count):
        part = value.astype(jnp.bfloat16)
        parts.append(part)
        value = value - part.astype(jnp.float32)
    return parts


PAIRS = {2: ((0, 0), (0, 1), (1, 0)), 3: ((0, 0), (0, 1), (1, 0), (1, 1), (0, 2), (2, 0))}


def lefts(value, count, dim):
    parts = bf16_parts(value, count)
    return jnp.concatenate([parts[a] for a, _ in PAIRS[count]], axis=dim)


def rights(value, count):
    parts = bf16_parts(value, count)
    return jnp.concatenate([parts[b] for _, b in PAIRS[count]], axis=0)


def products_kernel(tile_ref, left_ref, right_ref, gram_ref, out_ref):
    @pl.when(pl.program_id(0) == 0)
    def _():
        gram_ref[...] = jnp.zeros(gram_ref.shape, jnp.float32)
        out_ref[...] = jnp.zeros(out_ref.shape, jnp.float32)

    panel = jnp.concatenate([left_ref[...], right_ref[...]], axis=1)
    gram_ref[...] += dot(lefts(panel, 3, 0), rights(panel, 3), 0, 0)
    out_ref[...] += dot(lefts(tile_ref[...], 2, 0), rights(panel, 2), 0, 0)


def products(tile, left, right):
    rows_dev, cols_dev = tile.shape
    lines = 2 * B
    return pl.pallas_call(
        products_kernel,
        out_shape=(
            jax.ShapeDtypeStruct((B, B), jnp.float32),
            jax.ShapeDtypeStruct((cols_dev, B), jnp.float32),
        ),
        grid=(rows_dev // lines,),
        in_specs=[
            pl.BlockSpec((lines, cols_dev), lambda k: (k, 0)),
            pl.BlockSpec((lines, B // 2), lambda k: (k, 0)),
            pl.BlockSpec((lines, B // 2), lambda k: (k, 0)),
        ],
        out_specs=(
            pl.BlockSpec((B, B), lambda k: (0, 0)),
            pl.BlockSpec((cols_dev, B), lambda k: (0, 0)),
        ),
        cost_estimate=pl.CostEstimate(
            flops=6 * rows_dev * (cols_dev + 2 * B) * B,
            bytes_accessed=4 * rows_dev * (cols_dev + B),
            transcendentals=0,
        ),
        interpret=INTERPRET,
        name="products",
    )(tile, left, right)


def update_kernel(
    at_ref, tile_ref, pl_ref, pr_ref, ul_ref, ur_ref, f_ref, w_ref, tv_ref, r_ref, rt_ref, out_ref, factors
):
    row_at, col_at = at_ref[0], at_ref[1]
    step = pl.program_id(0)
    six = 6 * B

    @pl.when(step == 0)
    def _():
        factors[:six, :] = rights(f_ref[...], 3)
        factors[six:, :] = rights(tv_ref[...], 2)

    panel = jnp.concatenate([pl_ref[...], pr_ref[...]], axis=1)
    u_mat = jnp.concatenate([ul_ref[...], ur_ref[...]], axis=1)
    both = jnp.concatenate([lefts(panel, 3, 1), lefts(u_mat, 2, 1)], axis=1)
    out_ref[...] = tile_ref[...] - dot(both, factors[...], 1, 0)

    @pl.when((row_at == 0) & (step == 1))
    def _():
        out_ref[...] = out_ref[...] + w_ref[...]

    top = (row_at == 0) & (step == 0)

    @pl.when((col_at == 0) & jnp.logical_not(top))
    def _():
        out_ref[:, :B] = jnp.zeros((B, B), jnp.float32)

    @pl.when((col_at == 0) & (row_at == 0) & (step == 1))
    def _():
        out_ref[:, :B] = r_ref[...]

    @pl.when(top & (col_at == 0))
    def _():
        out_ref[:, B:] = rt_ref[:, : B // 2]

    @pl.when(top & (col_at == 1))
    def _():
        out_ref[:, : B // 2] = rt_ref[:, B // 2 :]
        out_ref[:, B // 2 :] = jnp.zeros((B, B), jnp.float32)

    @pl.when(top & (col_at >= 2))
    def _():
        out_ref[...] = jnp.zeros(out_ref.shape, jnp.float32)


def updated(at, tile, panel, u_mat, small, upper):
    rows_dev, cols_dev = tile.shape

    def whole(shape):
        return pl.BlockSpec(shape, lambda k, at: (0, 0))

    def lines(width):
        return pl.BlockSpec((B, width), lambda k, at: (k, 0))

    return pl.pallas_call(
        update_kernel,
        out_shape=jax.ShapeDtypeStruct(tile.shape, jnp.float32),
        grid_spec=pltpu.PrefetchScalarGridSpec(
            num_scalar_prefetch=1,
            grid=(rows_dev // B,),
            in_specs=[lines(cols_dev)]
            + [lines(B // 2)] * 4
            + [whole((B, cols_dev))] * 3
            + [whole((B, B))] * 2,
            out_specs=lines(cols_dev),
            scratch_shapes=[pltpu.VMEM((9 * B, cols_dev), jnp.bfloat16)],
        ),
        cost_estimate=pl.CostEstimate(
            flops=9 * 2 * rows_dev * cols_dev * B,
            bytes_accessed=4 * rows_dev * (2 * cols_dev + 2 * B),
            transcendentals=0,
        ),
        interpret=INTERPRET,
        name="update",
    )(at, tile, *panel, *u_mat, *small, upper, upper.T)


def per_device(tile):
    _, cols_dev = tile.shape
    row_at = lax.axis_index(ROW)
    col_at = lax.axis_index(COL)
    global_cols = col_at * cols_dev + jnp.arange(cols_dev, dtype=jnp.int32)
    band = jnp.arange(B, dtype=jnp.int32)
    zero = jnp.float32(0.0)

    place = (
        lax.axis_index("c") * 16 + lax.axis_index("y") * 4 + lax.axis_index("zl")
    )
    at = jnp.stack([row_at, col_at]).astype(jnp.int32)

    strip = jnp.where((global_cols >= B)[:, None], tile[:B, :].T, zero)
    panel_part = spread_strip(strip.reshape(8, -1, B))
    panel = plane_gather(panel_part)

    gram, product = products(tile, *panel)
    gram_slice = lax.dynamic_slice_in_dim(gram, place * 8, 8, 0)
    lead_slice = jnp.concatenate(
        [lax.dynamic_slice_in_dim(half, B + place * 8, 8, 0) for half in panel], axis=1
    )
    lead_slice = jnp.where(row_at == 0, lead_slice, zero)
    message = jnp.concatenate([gram_slice, lead_slice], axis=0)
    message = jnp.concatenate(
        [product.reshape(8, -1, B), jnp.broadcast_to(message[None], (8, 16, B))], axis=1
    )
    message = lax.all_to_all(message, ROW, 0, 0, tiled=True)
    message = message.sum(axis=0)
    product_part, message = message[:-16], message[-16:]
    message = from_everyone(from_everyone(message, ("y", "zl")), "c")
    message = message.reshape(32, 2, 8, B)
    gram = message[:, 0].reshape(B, B)
    lead = message[:, 1].reshape(B, B)

    both = jnp.concatenate([strip, tile[B : 2 * B, :].T], axis=1).reshape(8, -1, 2 * B)
    both, gram = lax.optimization_barrier((both, gram))
    both = lax.all_to_all(both, ROW, 0, 0, tiled=True)
    both = both.reshape(8, -1, 2 * B)[0]
    upper, inverse = chol(gram)

    u_part = contract(product_part, inverse, 1, 1) - both[:, B:]
    u_there = lax.ppermute(u_part, ALL, TO_PLANE)
    both_j = row_gather(jnp.concatenate([both[:, :B], u_part], axis=1))
    t_mat = t_inverse(lead, inverse)
    unit_j = (global_cols[:, None] - B == band[None, :]).astype(jnp.float32)
    reflector_j = contract(both_j[:, :B], inverse, 1, 1) - unit_j
    u_j = both_j[:, B:]

    core_part = contract(reflector_j, u_j, 0, 0).reshape(32, 8, B)
    u_there, core_part = lax.optimization_barrier((u_there, core_part))
    core_part = lax.all_to_all(core_part, COL, 0, 0, tiled=True)
    core_part = core_part.reshape(32, 8, B).sum(axis=0)
    u_left, u_right, core_part = plane_gather(u_there, core_part)
    core_sum = from_everyone(core_part, COL).reshape(B, B)
    middle = contract(contract(t_mat, core_sum, 1, 0), t_mat, 1, 1)

    t_reflector_trans = contract(t_mat, reflector_j, 0, 1)
    w_trans = contract(t_mat, u_j, 1, 1) - contract(middle, reflector_j, 1, 1)
    first_trans = contract(inverse, w_trans, 0, 0)
    return updated(
        at,
        tile,
        panel,
        (u_left, u_right),
        (first_trans, w_trans, t_reflector_trans),
        upper * jnp.float32(1.0 / math.sqrt(N)),
    )


def solution(mesh):
    split = Mesh(mesh.devices.reshape(4, 2, 4, 4, 2), ALL)
    return jax.shard_map(
        per_device,
        mesh=split,
        in_specs=(P(ROW, COL),),
        out_specs=P(ROW, COL),
        check_vma=False,
    )
```

```python
import math

import jax
import jax.numpy as jnp
from jax import lax
from jax.experimental import pallas as pl
from jax.experimental.pallas import tpu as pltpu
from jax.sharding import Mesh
from jax.sharding import PartitionSpec as P


N = 12288
B = 256
ROW = ("x", "zh")
COL = ("y", "zl", "c")
ALL = ROW + COL
SIZES = {"x": 4, "zh": 2, "y": 4, "zl": 4, "c": 2}
HIGHEST = lax.Precision.HIGHEST
INTERPRET = False
STEP = 64
LINES = 768


def contract(left_op, right_op, left_dim, right_dim, precision=HIGHEST):
    return lax.dot_general(
        left_op,
        right_op,
        (((left_dim,), (right_dim,)), ((), ())),
        precision=precision,
        preferred_element_type=jnp.float32,
    )


def shifted(value, axis, by):
    size = SIZES[axis]
    return lax.ppermute(value, axis, [(k, (k + by) % size) for k in range(size)])


def gather_over(value, axis, dim=0):
    size = SIZES[axis]
    me = lax.axis_index(axis)
    out = jnp.zeros(value.shape[:dim] + (size,) + value.shape[dim:], value.dtype)
    for by in range(size):
        part = value if by == 0 else shifted(value, axis, by)
        out = lax.dynamic_update_index_in_dim(out, part, (me - by) % size, dim)
    return out


def from_everyone(value, axis):
    size = lax.axis_size(axis)
    return lax.all_to_all(
        jnp.broadcast_to(value[None], (size, *value.shape)), axis, 0, 0, tiled=True
    )


def plane_gather(piece, tied=None):
    rows, width = piece.shape
    half = width // 2
    left = gather_over(piece[:, :half], "y")
    right = gather_over(piece[:, half:], "zl")
    if tied is not None:
        left, right, tied = lax.optimization_barrier((left, right, tied))
    left = gather_over(left, "zl", 1)
    right = gather_over(right, "y", 0)
    left = gather_over(left.reshape(16 * rows, half), "c")
    right = gather_over(right.reshape(16 * rows, half), "c")
    left, right = left.reshape(32 * rows, half), right.reshape(32 * rows, half)
    return (left, right) if tied is None else (left, right, tied)


def row_gather(value):
    return from_everyone(value, ROW).reshape(8 * value.shape[0], value.shape[1])


def plane_place(piece):
    core, rest = divmod(piece, 16)
    return (rest // 4) * 8 + (rest % 4) * 2 + core


TO_PLANE = [
    (r * 32 + j, (j // 4) * 32 + plane_place((j % 4) * 8 + r)) for r in range(8) for j in range(32)
]
TO_ROWS = [(there, here) for here, there in TO_PLANE]


def spread_strip(parts):
    total = None
    for r in range(8):
        moves = [(j, (j // 4) * 32 + plane_place((j % 4) * 8 + r)) for j in range(32)]
        got = lax.ppermute(parts[r], ALL, moves)
        total = got if total is None else total + got
    return total


def mxu(left, right, left_dim=1, right_dim=0):
    return contract(left, right, left_dim, right_dim)


PANEL = 8


def panel_columns(work, at):
    return [
        jnp.broadcast_to(work[:, at + k : at + k + 1], work.shape) for k in range(PANEL)
    ]


def small_chol_inverse(block):
    size = block.shape[0]
    work = jnp.concatenate([block, eye_of(size)], axis=1)
    rows = lax.broadcasted_iota(jnp.int32, (size, 2 * size), 0)
    for at in range(0, size, PANEL):
        columns = panel_columns(work, at)
        for a in range(PANEL):
            k = at + a
            root = lax.rsqrt(columns[a][k : k + 1, :])
            factor = columns[a] * root
            for b in range(a + 1, PANEL):
                columns[b] = columns[b] - factor * factor[at + b : at + b + 1, :]
            line = work[k : k + 1, :] * root
            updated = work - factor * line
            work = jnp.where(rows == k, line, jnp.where(rows > k, updated, work))
    return work[:, size:]


def small_inverse(block):
    size = block.shape[0]
    work = jnp.concatenate([block, eye_of(size)], axis=1)
    rows = lax.broadcasted_iota(jnp.int32, (size, 2 * size), 0)
    for at in range(0, size, PANEL):
        columns = panel_columns(work, at)
        for a in range(PANEL):
            k = at + a
            scale = 1.0 / columns[a][k : k + 1, :]
            factor = jnp.where(rows == k, 1.0, columns[a])
            keep = rows != k
            for b in range(a + 1, PANEL):
                top = columns[b][k : k + 1, :] * scale
                columns[b] = jnp.where(keep, columns[b], 0.0) - jnp.where(
                    keep, factor, -1.0
                ) * top
            line = work[k : k + 1, :] * scale
            work = jnp.where(keep, work - factor * line, line)
    return work[:, size:]


def eye_of(size):
    rows = lax.broadcasted_iota(jnp.int32, (size, size), 0)
    cols = lax.broadcasted_iota(jnp.int32, (size, size), 1)
    return jnp.where(rows == cols, 1.0, 0.0).astype(jnp.float32)


def turned_left(value, by):
    return pltpu.roll(value, (B - by) % B, 1)[:, :STEP]


def chol_kernel(gram_ref, upper_ref, inverse_ref, work):
    lanes = lax.broadcasted_iota(jnp.int32, (STEP, B), 1)
    work[:, :B] = gram_ref[...]
    work[:, B:] = eye_of(B)

    def step(block, carry):
        at = pl.multiple_of(block * STEP, STEP)
        own = work[pl.ds(at, STEP), :]
        inv = small_chol_inverse(turned_left(own[:, :B], at))
        lines = mxu(inv, own)
        work[pl.ds(at, STEP), :] = lines
        ahead = jnp.where(lanes >= at + STEP, lines[:, :B], 0.0)
        work[...] = work[...] - mxu(ahead, lines, 0, 0)
        return carry

    lax.fori_loop(0, B // STEP, step, 0)
    rows = lax.broadcasted_iota(jnp.int32, (B, B), 0)
    cols = lax.broadcasted_iota(jnp.int32, (B, B), 1)
    upper_ref[...] = jnp.where(cols >= rows, work[:, :B], 0.0)
    inverse_ref[...] = jnp.where(cols <= rows, work[:, B:], 0.0)


def t_kernel(lead_ref, inverse_ref, t_ref, work):
    tall = lax.broadcasted_iota(jnp.int32, (B, STEP), 0)
    work[:, :B] = eye_of(B) - mxu(lead_ref[...], inverse_ref[...], 1, 1)
    work[:, B:] = eye_of(B)

    def step(block, carry):
        at = pl.multiple_of(block * STEP, STEP)
        turned = turned_left(work[:, :B], at)
        own = work[pl.ds(at, STEP), :]
        inv = small_inverse(turned_left(own[:, :B], at))
        lines = mxu(inv, own)
        others = jnp.where((tall < at) | (tall >= at + STEP), turned, 0.0)
        work[...] = work[...] - mxu(others, lines)
        work[pl.ds(at, STEP), :] = lines
        return carry

    lax.fori_loop(0, B // STEP, step, 0)
    t_ref[...] = work[:, B:]


def on_squares(kernel, outputs, *operands):
    square = jax.ShapeDtypeStruct((B, B), jnp.float32)
    vmem = pl.BlockSpec(memory_space=pltpu.VMEM)
    return pl.pallas_call(
        kernel,
        out_shape=(square,) * outputs,
        in_specs=[vmem] * len(operands),
        out_specs=(vmem,) * outputs,
        scratch_shapes=[pltpu.VMEM((B, 2 * B), jnp.float32)],
        cost_estimate=pl.CostEstimate(
            flops=2_000_000_000, bytes_accessed=4 * B * B * 4, transcendentals=0
        ),
        interpret=INTERPRET,
    )(*operands)


def chol(gram):
    return on_squares(chol_kernel, 2, gram)


def t_inverse(lead, inverse):
    return on_squares(t_kernel, 1, lead, inverse)[0]


def dot(left, right, left_dim, right_dim):
    return lax.dot_general(
        left, right, (((left_dim,), (right_dim,)), ((), ())), preferred_element_type=jnp.float32
    )


def bf16_parts(value, count):
    parts = []
    for _ in range(count):
        part = value.astype(jnp.bfloat16)
        parts.append(part)
        value = value - part.astype(jnp.float32)
    return parts


PAIRS = {2: ((0, 0), (0, 1), (1, 0)), 3: ((0, 0), (0, 1), (1, 0), (1, 1), (0, 2), (2, 0))}


def lefts(value, count, dim):
    parts = bf16_parts(value, count)
    return jnp.concatenate([parts[a] for a, _ in PAIRS[count]], axis=dim)


def rights(value, count):
    parts = bf16_parts(value, count)
    return jnp.concatenate([parts[b] for _, b in PAIRS[count]], axis=0)


def products_kernel(tile_ref, left_ref, right_ref, gram_ref, out_ref):
    @pl.when(pl.program_id(0) == 0)
    def _():
        gram_ref[...] = jnp.zeros(gram_ref.shape, jnp.float32)
        out_ref[...] = jnp.zeros(out_ref.shape, jnp.float32)

    panel = jnp.concatenate([left_ref[...], right_ref[...]], axis=1)
    gram_ref[...] += dot(lefts(panel, 3, 0), rights(panel, 3), 0, 0)
    out_ref[...] += dot(lefts(tile_ref[...], 2, 0), rights(panel, 2), 0, 0)


def products(tile, left, right):
    rows_dev, cols_dev = tile.shape
    lines = LINES
    return pl.pallas_call(
        products_kernel,
        out_shape=(
            jax.ShapeDtypeStruct((B, B), jnp.float32),
            jax.ShapeDtypeStruct((cols_dev, B), jnp.float32),
        ),
        grid=(rows_dev // lines,),
        in_specs=[
            pl.BlockSpec((lines, cols_dev), lambda k: (k, 0)),
            pl.BlockSpec((lines, B // 2), lambda k: (k, 0)),
            pl.BlockSpec((lines, B // 2), lambda k: (k, 0)),
        ],
        out_specs=(
            pl.BlockSpec((B, B), lambda k: (0, 0)),
            pl.BlockSpec((cols_dev, B), lambda k: (0, 0)),
        ),
        cost_estimate=pl.CostEstimate(
            flops=6 * rows_dev * (cols_dev + 2 * B) * B,
            bytes_accessed=4 * rows_dev * (cols_dev + B),
            transcendentals=0,
        ),
        interpret=INTERPRET,
        name="products",
    )(tile, left, right)


def update_kernel(
    at_ref, tile_ref, pl_ref, pr_ref, ul_ref, ur_ref, f_ref, w_ref, tv_ref, r_ref, rt_ref, out_ref, factors
):
    row_at, col_at = at_ref[0], at_ref[1]
    step = pl.program_id(0)
    six = 6 * B

    @pl.when(step == 0)
    def _():
        factors[:six, :] = rights(f_ref[...], 3)
        factors[six:, :] = rights(tv_ref[...], 2)

    panel = jnp.concatenate([pl_ref[...], pr_ref[...]], axis=1)
    u_mat = jnp.concatenate([ul_ref[...], ur_ref[...]], axis=1)
    both = jnp.concatenate([lefts(panel, 3, 1), lefts(u_mat, 2, 1)], axis=1)
    out_ref[...] = tile_ref[...] - dot(both, factors[...], 1, 0)

    top = (row_at == 0) & (step == 0)

    @pl.when(top)
    def _():
        out_ref[B : 2 * B, :] = out_ref[B : 2 * B, :] + w_ref[...]

    @pl.when((col_at == 0) & jnp.logical_not(top))
    def _():
        out_ref[:, :B] = jnp.zeros((LINES, B), jnp.float32)

    @pl.when((col_at == 0) & top)
    def _():
        out_ref[B : 2 * B, :B] = r_ref[...]
        out_ref[2 * B :, :B] = jnp.zeros((LINES - 2 * B, B), jnp.float32)
        out_ref[:B, B:] = rt_ref[:, : B // 2]

    @pl.when((col_at == 1) & top)
    def _():
        out_ref[:B, : B // 2] = rt_ref[:, B // 2 :]
        out_ref[:B, B // 2 :] = jnp.zeros((B, B), jnp.float32)

    @pl.when((col_at >= 2) & top)
    def _():
        out_ref[:B, :] = jnp.zeros((B, out_ref.shape[1]), jnp.float32)


def updated(at, tile, panel, u_mat, small, upper):
    rows_dev, cols_dev = tile.shape

    def whole(shape):
        return pl.BlockSpec(shape, lambda k, at: (0, 0))

    def lines(width):
        return pl.BlockSpec((LINES, width), lambda k, at: (k, 0))

    return pl.pallas_call(
        update_kernel,
        out_shape=jax.ShapeDtypeStruct(tile.shape, jnp.float32),
        grid_spec=pltpu.PrefetchScalarGridSpec(
            num_scalar_prefetch=1,
            grid=(rows_dev // LINES,),
            in_specs=[lines(cols_dev)]
            + [lines(B // 2)] * 4
            + [whole((B, cols_dev))] * 3
            + [whole((B, B))] * 2,
            out_specs=lines(cols_dev),
            scratch_shapes=[pltpu.VMEM((9 * B, cols_dev), jnp.bfloat16)],
        ),
        cost_estimate=pl.CostEstimate(
            flops=9 * 2 * rows_dev * cols_dev * B,
            bytes_accessed=4 * rows_dev * (2 * cols_dev + 2 * B),
            transcendentals=0,
        ),
        interpret=INTERPRET,
        name="update",
    )(at, tile, *panel, *u_mat, *small, upper, upper.T)


def per_device(tile):
    _, cols_dev = tile.shape
    row_at = lax.axis_index(ROW)
    col_at = lax.axis_index(COL)
    global_cols = col_at * cols_dev + jnp.arange(cols_dev, dtype=jnp.int32)
    band = jnp.arange(B, dtype=jnp.int32)
    zero = jnp.float32(0.0)

    place = (
        lax.axis_index("c") * 16 + lax.axis_index("y") * 4 + lax.axis_index("zl")
    )
    at = jnp.stack([row_at, col_at]).astype(jnp.int32)

    strip = jnp.where((global_cols >= B)[:, None], tile[:B, :].T, zero)
    panel_part = spread_strip(strip.reshape(8, -1, B))
    panel = plane_gather(panel_part)

    panel_part, *panel = lax.optimization_barrier((panel_part, *panel))
    panel_there = lax.ppermute(panel_part, ALL, TO_ROWS)
    gram, product = products(tile, *panel)
    gram_slice = lax.dynamic_slice_in_dim(gram, place * 8, 8, 0)
    lead_slice = jnp.concatenate(
        [lax.dynamic_slice_in_dim(half, B + place * 8, 8, 0) for half in panel], axis=1
    )
    lead_slice = jnp.where(row_at == 0, lead_slice, zero)
    message = jnp.concatenate([gram_slice, lead_slice], axis=0)
    message = jnp.concatenate(
        [product.reshape(8, -1, B), jnp.broadcast_to(message[None], (8, 16, B))], axis=1
    )
    message = lax.all_to_all(message, ROW, 0, 0, tiled=True)
    message = message.sum(axis=0)
    product_part, message = message[:-16], message[-16:]
    message = from_everyone(from_everyone(message, ("y", "zl")), "c")
    message = message.reshape(32, 2, 8, B)
    gram = message[:, 0].reshape(B, B)
    lead = message[:, 1].reshape(B, B)

    edge = tile[B : 2 * B, :].T.reshape(8, -1, B)
    edge, gram = lax.optimization_barrier((edge, gram))
    edge = lax.all_to_all(edge, ROW, 0, 0, tiled=True)
    edge = edge.reshape(8, -1, B)[0]
    upper, inverse = chol(gram)

    u_part = contract(product_part, inverse, 1, 1) - edge
    u_there = lax.ppermute(u_part, ALL, TO_PLANE)
    both_j = row_gather(jnp.concatenate([panel_there, u_part], axis=1))
    t_mat = t_inverse(lead, inverse)
    unit_j = (global_cols[:, None] - B == band[None, :]).astype(jnp.float32)
    reflector_j = contract(both_j[:, :B], inverse, 1, 1) - unit_j
    u_j = both_j[:, B:]

    core_part = contract(reflector_j, u_j, 0, 0).reshape(32, 8, B)
    u_there, core_part = lax.optimization_barrier((u_there, core_part))
    core_part = lax.all_to_all(core_part, COL, 0, 0, tiled=True)
    core_part = core_part.reshape(32, 8, B).sum(axis=0)
    u_left, u_right, core_part = plane_gather(u_there, core_part)
    core_sum = from_everyone(core_part, COL).reshape(B, B)
    middle = contract(contract(t_mat, core_sum, 1, 0), t_mat, 1, 1)

    t_reflector_trans = contract(t_mat, reflector_j, 0, 1)
    w_trans = contract(t_mat, u_j, 1, 1) - contract(middle, reflector_j, 1, 1)
    first_trans = contract(inverse, w_trans, 0, 0)
    return updated(
        at,
        tile,
        panel,
        (u_left, u_right),
        (first_trans, w_trans, t_reflector_trans),
        upper * jnp.float32(1.0 / math.sqrt(N)),
    )


def solution(mesh):
    split = Mesh(mesh.devices.reshape(4, 2, 4, 4, 2), ALL)
    return jax.shard_map(
        per_device,
        mesh=split,
        in_specs=(P(ROW, COL),),
        out_specs=P(ROW, COL),
        check_vma=False,
    )
```

```python
import math

import jax
import jax.numpy as jnp
from jax import lax
from jax.experimental import pallas as pl
from jax.experimental.pallas import tpu as pltpu
from jax.sharding import Mesh
from jax.sharding import PartitionSpec as P


N = 12288
B = 256
ROW = ("x", "zh")
COL = ("y", "zl", "c")
ALL = ROW + COL
SIZES = {"x": 4, "zh": 2, "y": 4, "zl": 4, "c": 2}
HIGHEST = lax.Precision.HIGHEST
INTERPRET = False
STEP = 64
LINES = 768


def contract(left_op, right_op, left_dim, right_dim, precision=HIGHEST):
    return lax.dot_general(
        left_op,
        right_op,
        (((left_dim,), (right_dim,)), ((), ())),
        precision=precision,
        preferred_element_type=jnp.float32,
    )


def shifted(value, axis, by):
    size = SIZES[axis]
    return lax.ppermute(value, axis, [(k, (k + by) % size) for k in range(size)])


def gather_over(value, axis, dim=0):
    size = SIZES[axis]
    me = lax.axis_index(axis)
    out = jnp.zeros(value.shape[:dim] + (size,) + value.shape[dim:], value.dtype)
    for by in range(size):
        part = value if by == 0 else shifted(value, axis, by)
        out = lax.dynamic_update_index_in_dim(out, part, (me - by) % size, dim)
    return out


def from_everyone(value, axis):
    size = lax.axis_size(axis)
    return lax.all_to_all(
        jnp.broadcast_to(value[None], (size, *value.shape)), axis, 0, 0, tiled=True
    )


def plane_gather(piece, tied=None):
    rows, width = piece.shape
    half = width // 2
    left = gather_over(piece[:, :half], "y")
    right = gather_over(piece[:, half:], "zl")
    if tied is not None:
        left, right, tied = lax.optimization_barrier((left, right, tied))
    left = gather_over(left, "zl", 1)
    right = gather_over(right, "y", 0)
    left = gather_over(left.reshape(16 * rows, half), "c")
    right = gather_over(right.reshape(16 * rows, half), "c")
    left, right = left.reshape(32 * rows, half), right.reshape(32 * rows, half)
    return (left, right) if tied is None else (left, right, tied)


def row_gather(value):
    return from_everyone(value, ROW).reshape(8 * value.shape[0], value.shape[1])


def plane_place(piece):
    core, rest = divmod(piece, 16)
    return (rest // 4) * 8 + (rest % 4) * 2 + core


TO_PLANE = [
    (r * 32 + j, (j // 4) * 32 + plane_place((j % 4) * 8 + r)) for r in range(8) for j in range(32)
]


def from_first(parts):
    return lax.all_to_all(parts, ROW, 0, 0, tiled=True).reshape(parts.shape)[0]


def mxu(left, right, left_dim=1, right_dim=0):
    return contract(left, right, left_dim, right_dim)


PANEL = 8


def panel_columns(work, at):
    return [
        jnp.broadcast_to(work[:, at + k : at + k + 1], work.shape) for k in range(PANEL)
    ]


def small_chol_inverse(block):
    size = block.shape[0]
    work = jnp.concatenate([block, eye_of(size)], axis=1)
    rows = lax.broadcasted_iota(jnp.int32, (size, 2 * size), 0)
    for at in range(0, size, PANEL):
        columns = panel_columns(work, at)
        for a in range(PANEL):
            k = at + a
            root = lax.rsqrt(columns[a][k : k + 1, :])
            factor = columns[a] * root
            for b in range(a + 1, PANEL):
                columns[b] = columns[b] - factor * factor[at + b : at + b + 1, :]
            line = work[k : k + 1, :] * root
            updated = work - factor * line
            work = jnp.where(rows == k, line, jnp.where(rows > k, updated, work))
    return work[:, size:]


def small_inverse(block):
    size = block.shape[0]
    work = jnp.concatenate([block, eye_of(size)], axis=1)
    rows = lax.broadcasted_iota(jnp.int32, (size, 2 * size), 0)
    for at in range(0, size, PANEL):
        columns = panel_columns(work, at)
        for a in range(PANEL):
            k = at + a
            scale = 1.0 / columns[a][k : k + 1, :]
            factor = jnp.where(rows == k, 1.0, columns[a])
            keep = rows != k
            for b in range(a + 1, PANEL):
                top = columns[b][k : k + 1, :] * scale
                columns[b] = jnp.where(keep, columns[b], 0.0) - jnp.where(
                    keep, factor, -1.0
                ) * top
            line = work[k : k + 1, :] * scale
            work = jnp.where(keep, work - factor * line, line)
    return work[:, size:]


def eye_of(size):
    rows = lax.broadcasted_iota(jnp.int32, (size, size), 0)
    cols = lax.broadcasted_iota(jnp.int32, (size, size), 1)
    return jnp.where(rows == cols, 1.0, 0.0).astype(jnp.float32)


def turned_left(value, by):
    return pltpu.roll(value, (B - by) % B, 1)[:, :STEP]


def chol_kernel(gram_ref, upper_ref, inverse_ref, work):
    lanes = lax.broadcasted_iota(jnp.int32, (STEP, B), 1)
    work[:, :B] = gram_ref[...]
    work[:, B:] = eye_of(B)

    def step(block, carry):
        at = pl.multiple_of(block * STEP, STEP)
        own = work[pl.ds(at, STEP), :]
        inv = small_chol_inverse(turned_left(own[:, :B], at))
        lines = mxu(inv, own)
        work[pl.ds(at, STEP), :] = lines
        ahead = jnp.where(lanes >= at + STEP, lines[:, :B], 0.0)
        work[...] = work[...] - mxu(ahead, lines, 0, 0)
        return carry

    lax.fori_loop(0, B // STEP, step, 0)
    rows = lax.broadcasted_iota(jnp.int32, (B, B), 0)
    cols = lax.broadcasted_iota(jnp.int32, (B, B), 1)
    upper_ref[...] = jnp.where(cols >= rows, work[:, :B], 0.0)
    inverse_ref[...] = jnp.where(cols <= rows, work[:, B:], 0.0)


def t_kernel(lead_ref, inverse_ref, t_ref, work):
    tall = lax.broadcasted_iota(jnp.int32, (B, STEP), 0)
    work[:, :B] = eye_of(B) - mxu(lead_ref[...], inverse_ref[...], 1, 1)
    work[:, B:] = eye_of(B)

    def step(block, carry):
        at = pl.multiple_of(block * STEP, STEP)
        turned = turned_left(work[:, :B], at)
        own = work[pl.ds(at, STEP), :]
        inv = small_inverse(turned_left(own[:, :B], at))
        lines = mxu(inv, own)
        others = jnp.where((tall < at) | (tall >= at + STEP), turned, 0.0)
        work[...] = work[...] - mxu(others, lines)
        work[pl.ds(at, STEP), :] = lines
        return carry

    lax.fori_loop(0, B // STEP, step, 0)
    t_ref[...] = work[:, B:]


def on_squares(kernel, outputs, *operands):
    square = jax.ShapeDtypeStruct((B, B), jnp.float32)
    vmem = pl.BlockSpec(memory_space=pltpu.VMEM)
    return pl.pallas_call(
        kernel,
        out_shape=(square,) * outputs,
        in_specs=[vmem] * len(operands),
        out_specs=(vmem,) * outputs,
        scratch_shapes=[pltpu.VMEM((B, 2 * B), jnp.float32)],
        cost_estimate=pl.CostEstimate(
            flops=2_000_000_000, bytes_accessed=4 * B * B * 4, transcendentals=0
        ),
        interpret=INTERPRET,
    )(*operands)


def chol(gram):
    return on_squares(chol_kernel, 2, gram)


def t_inverse(lead, inverse):
    return on_squares(t_kernel, 1, lead, inverse)[0]


def dot(left, right, left_dim, right_dim):
    return lax.dot_general(
        left, right, (((left_dim,), (right_dim,)), ((), ())), preferred_element_type=jnp.float32
    )


def bf16_parts(value, count):
    parts = []
    for _ in range(count):
        part = value.astype(jnp.bfloat16)
        parts.append(part)
        value = value - part.astype(jnp.float32)
    return parts


PAIRS = {2: ((0, 0), (0, 1), (1, 0)), 3: ((0, 0), (0, 1), (1, 0), (1, 1), (0, 2), (2, 0))}


def lefts(value, count, dim):
    parts = bf16_parts(value, count)
    return jnp.concatenate([parts[a] for a, _ in PAIRS[count]], axis=dim)


def rights(value, count):
    parts = bf16_parts(value, count)
    return jnp.concatenate([parts[b] for _, b in PAIRS[count]], axis=0)


def products_kernel(tile_ref, left_ref, right_ref, gram_ref, out_ref):
    @pl.when(pl.program_id(0) == 0)
    def _():
        gram_ref[...] = jnp.zeros(gram_ref.shape, jnp.float32)
        out_ref[...] = jnp.zeros(out_ref.shape, jnp.float32)

    panel = jnp.concatenate([left_ref[...], right_ref[...]], axis=1)
    gram_ref[...] += dot(lefts(panel, 3, 0), rights(panel, 3), 0, 0)
    out_ref[...] += dot(lefts(tile_ref[...], 2, 0), rights(panel, 2), 0, 0)


def products(tile, left, right):
    rows_dev, cols_dev = tile.shape
    lines = LINES
    return pl.pallas_call(
        products_kernel,
        out_shape=(
            jax.ShapeDtypeStruct((B, B), jnp.float32),
            jax.ShapeDtypeStruct((cols_dev, B), jnp.float32),
        ),
        grid=(rows_dev // lines,),
        in_specs=[
            pl.BlockSpec((lines, cols_dev), lambda k: (k, 0)),
            pl.BlockSpec((lines, B // 2), lambda k: (k, 0)),
            pl.BlockSpec((lines, B // 2), lambda k: (k, 0)),
        ],
        out_specs=(
            pl.BlockSpec((B, B), lambda k: (0, 0)),
            pl.BlockSpec((cols_dev, B), lambda k: (0, 0)),
        ),
        cost_estimate=pl.CostEstimate(
            flops=6 * rows_dev * (cols_dev + 2 * B) * B,
            bytes_accessed=4 * rows_dev * (cols_dev + B),
            transcendentals=0,
        ),
        interpret=INTERPRET,
        name="products",
    )(tile, left, right)


def update_kernel(
    at_ref, tile_ref, pl_ref, pr_ref, ul_ref, ur_ref, f_ref, w_ref, tv_ref, r_ref, rt_ref, out_ref, factors
):
    row_at, col_at = at_ref[0], at_ref[1]
    step = pl.program_id(0)
    six = 6 * B

    @pl.when(step == 0)
    def _():
        factors[:six, :] = rights(f_ref[...], 3)
        factors[six:, :] = rights(tv_ref[...], 2)

    panel = jnp.concatenate([pl_ref[...], pr_ref[...]], axis=1)
    u_mat = jnp.concatenate([ul_ref[...], ur_ref[...]], axis=1)
    both = jnp.concatenate([lefts(panel, 3, 1), lefts(u_mat, 2, 1)], axis=1)
    out_ref[...] = tile_ref[...] - dot(both, factors[...], 1, 0)

    top = (row_at == 0) & (step == 0)

    @pl.when(top)
    def _():
        out_ref[B : 2 * B, :] = out_ref[B : 2 * B, :] + w_ref[...]

    @pl.when((col_at == 0) & jnp.logical_not(top))
    def _():
        out_ref[:, :B] = jnp.zeros((LINES, B), jnp.float32)

    @pl.when((col_at == 0) & top)
    def _():
        out_ref[B : 2 * B, :B] = r_ref[...]
        out_ref[2 * B :, :B] = jnp.zeros((LINES - 2 * B, B), jnp.float32)
        out_ref[:B, B:] = rt_ref[:, : B // 2]

    @pl.when((col_at == 1) & top)
    def _():
        out_ref[:B, : B // 2] = rt_ref[:, B // 2 :]
        out_ref[:B, B // 2 :] = jnp.zeros((B, B), jnp.float32)

    @pl.when((col_at >= 2) & top)
    def _():
        out_ref[:B, :] = jnp.zeros((B, out_ref.shape[1]), jnp.float32)


def updated(at, tile, panel, u_mat, small, upper):
    rows_dev, cols_dev = tile.shape

    def whole(shape):
        return pl.BlockSpec(shape, lambda k, at: (0, 0))

    def lines(width):
        return pl.BlockSpec((LINES, width), lambda k, at: (k, 0))

    return pl.pallas_call(
        update_kernel,
        out_shape=jax.ShapeDtypeStruct(tile.shape, jnp.float32),
        grid_spec=pltpu.PrefetchScalarGridSpec(
            num_scalar_prefetch=1,
            grid=(rows_dev // LINES,),
            in_specs=[lines(cols_dev)]
            + [lines(B // 2)] * 4
            + [whole((B, cols_dev))] * 3
            + [whole((B, B))] * 2,
            out_specs=lines(cols_dev),
            scratch_shapes=[pltpu.VMEM((9 * B, cols_dev), jnp.bfloat16)],
        ),
        cost_estimate=pl.CostEstimate(
            flops=9 * 2 * rows_dev * cols_dev * B,
            bytes_accessed=4 * rows_dev * (2 * cols_dev + 2 * B),
            transcendentals=0,
        ),
        interpret=INTERPRET,
        name="update",
    )(at, tile, *panel, *u_mat, *small, upper, upper.T)


def per_device(tile):
    _, cols_dev = tile.shape
    row_at = lax.axis_index(ROW)
    col_at = lax.axis_index(COL)
    global_cols = col_at * cols_dev + jnp.arange(cols_dev, dtype=jnp.int32)
    band = jnp.arange(B, dtype=jnp.int32)
    zero = jnp.float32(0.0)

    place = (
        lax.axis_index("c") * 16 + lax.axis_index("y") * 4 + lax.axis_index("zl")
    )
    at = jnp.stack([row_at, col_at]).astype(jnp.int32)

    strip = jnp.where((global_cols >= B)[:, None], tile[:B, :].T, zero)
    panel_there = from_first(strip.reshape(8, -1, B))
    panel_part = lax.ppermute(panel_there, ALL, TO_PLANE)
    panel = plane_gather(panel_part)

    gram, product = products(tile, *panel)
    gram_slice = lax.dynamic_slice_in_dim(gram, place * 8, 8, 0)
    lead_slice = jnp.concatenate(
        [lax.dynamic_slice_in_dim(half, B + place * 8, 8, 0) for half in panel], axis=1
    )
    lead_slice = jnp.where(row_at == 0, lead_slice, zero)
    message = jnp.concatenate([gram_slice, lead_slice], axis=0)
    message = jnp.concatenate(
        [product.reshape(8, -1, B), jnp.broadcast_to(message[None], (8, 16, B))], axis=1
    )
    message = lax.all_to_all(message, ROW, 0, 0, tiled=True)
    message = message.sum(axis=0)
    product_part, message = message[:-16], message[-16:]
    message = from_everyone(from_everyone(message, ("y", "zl")), "c")
    message = message.reshape(32, 2, 8, B)
    gram = message[:, 0].reshape(B, B)
    lead = message[:, 1].reshape(B, B)

    edge = tile[B : 2 * B, :].T.reshape(8, -1, B)
    edge, gram = lax.optimization_barrier((edge, gram))
    edge = from_first(edge)
    upper, inverse = chol(gram)

    part = panel_there.shape[0]
    both = contract(jnp.concatenate([panel_there, product_part], axis=0), inverse, 1, 1)
    part_rows = col_at * cols_dev + row_at * part + jnp.arange(part, dtype=jnp.int32)
    unit_part = (part_rows[:, None] - B == band[None, :]).astype(jnp.float32)
    u_part = both[part:] - edge
    u_there = lax.ppermute(u_part, ALL, TO_PLANE)
    both_j = row_gather(jnp.concatenate([both[:part] - unit_part, u_part], axis=1))
    t_mat = t_inverse(lead, inverse)
    reflector_j, u_j = both_j[:, :B], both_j[:, B:]

    core_part = contract(reflector_j, u_j, 0, 0).reshape(32, 8, B)
    u_there, core_part = lax.optimization_barrier((u_there, core_part))
    core_part = lax.all_to_all(core_part, COL, 0, 0, tiled=True)
    core_part = core_part.reshape(32, 8, B).sum(axis=0)
    u_left, u_right, core_part = plane_gather(u_there, core_part)
    core_sum = from_everyone(core_part, COL).reshape(B, B)
    middle = contract(contract(t_mat, core_sum, 1, 0), t_mat, 1, 1)

    t_reflector_trans = contract(t_mat, reflector_j, 0, 1)
    w_trans = contract(t_mat, u_j, 1, 1) - contract(middle, reflector_j, 1, 1)
    first_trans = contract(inverse, w_trans, 0, 0)
    return updated(
        at,
        tile,
        panel,
        (u_left, u_right),
        (first_trans, w_trans, t_reflector_trans),
        upper * jnp.float32(1.0 / math.sqrt(N)),
    )


def solution(mesh):
    split = Mesh(mesh.devices.reshape(4, 2, 4, 4, 2), ALL)
    return jax.shard_map(
        per_device,
        mesh=split,
        in_specs=(P(ROW, COL),),
        out_specs=P(ROW, COL),
        check_vma=False,
    )
```

```python
import math

import jax
import jax.numpy as jnp
from jax import lax
from jax.experimental import pallas as pl
from jax.experimental.pallas import tpu as pltpu
from jax.sharding import Mesh
from jax.sharding import PartitionSpec as P


N = 12288
B = 256
ROW = ("x", "zh")
COL = ("y", "zl", "c")
ALL = ROW + COL
SIZES = {"x": 4, "zh": 2, "y": 4, "zl": 4, "c": 2}
HIGHEST = lax.Precision.HIGHEST
INTERPRET = False
STEP = 64
LINES = 768


def contract(left_op, right_op, left_dim, right_dim, precision=HIGHEST):
    return lax.dot_general(
        left_op,
        right_op,
        (((left_dim,), (right_dim,)), ((), ())),
        precision=precision,
        preferred_element_type=jnp.float32,
    )


def shifted(value, axis, by):
    size = SIZES[axis]
    return lax.ppermute(value, axis, [(k, (k + by) % size) for k in range(size)])


def gather_over(value, axis, dim=0):
    size = SIZES[axis]
    me = lax.axis_index(axis)
    out = jnp.zeros(value.shape[:dim] + (size,) + value.shape[dim:], value.dtype)
    for by in range(size):
        part = value if by == 0 else shifted(value, axis, by)
        out = lax.dynamic_update_index_in_dim(out, part, (me - by) % size, dim)
    return out


def from_everyone(value, axis):
    size = lax.axis_size(axis)
    return lax.all_to_all(
        jnp.broadcast_to(value[None], (size, *value.shape)), axis, 0, 0, tiled=True
    )


def plane_gather(piece, tied=None):
    rows, width = piece.shape
    half = width // 2
    left = gather_over(piece[:, :half], "y")
    right = gather_over(piece[:, half:], "zl")
    if tied is not None:
        left, right, tied = lax.optimization_barrier((left, right, tied))
    left = gather_over(left, "zl", 1)
    right = gather_over(right, "y", 0)
    left = gather_over(left.reshape(16 * rows, half), "c")
    right = gather_over(right.reshape(16 * rows, half), "c")
    left, right = left.reshape(32 * rows, half), right.reshape(32 * rows, half)
    return (left, right) if tied is None else (left, right, tied)


def row_gather(value):
    return from_everyone(value, ROW).reshape(8 * value.shape[0], value.shape[1])


def plane_place(piece):
    core, rest = divmod(piece, 16)
    return (rest // 4) * 8 + (rest % 4) * 2 + core


TO_PLANE = [
    (r * 32 + j, (j // 4) * 32 + plane_place((j % 4) * 8 + r)) for r in range(8) for j in range(32)
]
TO_ROWS = [(there, here) for here, there in TO_PLANE]


def spread_strip(parts):
    total = None
    for r in range(8):
        moves = [(j, (j // 4) * 32 + plane_place((j % 4) * 8 + r)) for j in range(32)]
        got = lax.ppermute(parts[r], ALL, moves)
        total = got if total is None else total + got
    return total


def mxu(left, right, left_dim=1, right_dim=0):
    return contract(left, right, left_dim, right_dim)


PANEL = 8


def panel_columns(work, at):
    return [
        jnp.broadcast_to(work[:, at + k : at + k + 1], work.shape) for k in range(PANEL)
    ]


def small_chol_inverse(block):
    size = block.shape[0]
    work = jnp.concatenate([block, eye_of(size)], axis=1)
    rows = lax.broadcasted_iota(jnp.int32, (size, 2 * size), 0)
    for at in range(0, size, PANEL):
        columns = panel_columns(work, at)
        for a in range(PANEL):
            k = at + a
            root = lax.rsqrt(columns[a][k : k + 1, :])
            factor = columns[a] * root
            for b in range(a + 1, PANEL):
                columns[b] = columns[b] - factor * factor[at + b : at + b + 1, :]
            line = work[k : k + 1, :] * root
            updated = work - factor * line
            work = jnp.where(rows == k, line, jnp.where(rows > k, updated, work))
    return work[:, size:]


def small_inverse(block):
    size = block.shape[0]
    work = jnp.concatenate([block, eye_of(size)], axis=1)
    rows = lax.broadcasted_iota(jnp.int32, (size, 2 * size), 0)
    for at in range(0, size, PANEL):
        columns = panel_columns(work, at)
        for a in range(PANEL):
            k = at + a
            scale = 1.0 / columns[a][k : k + 1, :]
            factor = jnp.where(rows == k, 1.0, columns[a])
            keep = rows != k
            for b in range(a + 1, PANEL):
                top = columns[b][k : k + 1, :] * scale
                columns[b] = jnp.where(keep, columns[b], 0.0) - jnp.where(
                    keep, factor, -1.0
                ) * top
            line = work[k : k + 1, :] * scale
            work = jnp.where(keep, work - factor * line, line)
    return work[:, size:]


def eye_of(size):
    rows = lax.broadcasted_iota(jnp.int32, (size, size), 0)
    cols = lax.broadcasted_iota(jnp.int32, (size, size), 1)
    return jnp.where(rows == cols, 1.0, 0.0).astype(jnp.float32)


def turned_left(value, by):
    return pltpu.roll(value, (B - by) % B, 1)[:, :STEP]


def chol_kernel(gram_ref, upper_ref, inverse_ref, work):
    lanes = lax.broadcasted_iota(jnp.int32, (STEP, B), 1)
    work[:, :B] = gram_ref[...]
    work[:, B:] = eye_of(B)

    def step(block, carry):
        at = pl.multiple_of(block * STEP, STEP)
        own = work[pl.ds(at, STEP), :]
        inv = small_chol_inverse(turned_left(own[:, :B], at))
        lines = mxu(inv, own)
        work[pl.ds(at, STEP), :] = lines
        ahead = jnp.where(lanes >= at + STEP, lines[:, :B], 0.0)
        work[...] = work[...] - mxu(ahead, lines, 0, 0)
        return carry

    lax.fori_loop(0, B // STEP, step, 0)
    rows = lax.broadcasted_iota(jnp.int32, (B, B), 0)
    cols = lax.broadcasted_iota(jnp.int32, (B, B), 1)
    upper_ref[...] = jnp.where(cols >= rows, work[:, :B], 0.0)
    inverse_ref[...] = jnp.where(cols <= rows, work[:, B:], 0.0)


def t_kernel(lead_ref, inverse_ref, t_ref, work):
    tall = lax.broadcasted_iota(jnp.int32, (B, STEP), 0)
    work[:, :B] = eye_of(B) - mxu(lead_ref[...], inverse_ref[...], 1, 1)
    work[:, B:] = eye_of(B)

    def step(block, carry):
        at = pl.multiple_of(block * STEP, STEP)
        turned = turned_left(work[:, :B], at)
        own = work[pl.ds(at, STEP), :]
        inv = small_inverse(turned_left(own[:, :B], at))
        lines = mxu(inv, own)
        others = jnp.where((tall < at) | (tall >= at + STEP), turned, 0.0)
        work[...] = work[...] - mxu(others, lines)
        work[pl.ds(at, STEP), :] = lines
        return carry

    lax.fori_loop(0, B // STEP, step, 0)
    t_ref[...] = work[:, B:]


def on_squares(kernel, outputs, *operands):
    square = jax.ShapeDtypeStruct((B, B), jnp.float32)
    vmem = pl.BlockSpec(memory_space=pltpu.VMEM)
    return pl.pallas_call(
        kernel,
        out_shape=(square,) * outputs,
        in_specs=[vmem] * len(operands),
        out_specs=(vmem,) * outputs,
        scratch_shapes=[pltpu.VMEM((B, 2 * B), jnp.float32)],
        cost_estimate=pl.CostEstimate(
            flops=2_000_000_000, bytes_accessed=4 * B * B * 4, transcendentals=0
        ),
        interpret=INTERPRET,
    )(*operands)


def chol(gram):
    return on_squares(chol_kernel, 2, gram)


def t_inverse(lead, inverse):
    return on_squares(t_kernel, 1, lead, inverse)[0]


def dot(left, right, left_dim, right_dim):
    return lax.dot_general(
        left, right, (((left_dim,), (right_dim,)), ((), ())), preferred_element_type=jnp.float32
    )


def bf16_parts(value, count):
    parts = []
    for _ in range(count):
        part = value.astype(jnp.bfloat16)
        parts.append(part)
        value = value - part.astype(jnp.float32)
    return parts


PAIRS = {2: ((0, 0), (0, 1), (1, 0)), 3: ((0, 0), (0, 1), (1, 0), (1, 1), (0, 2), (2, 0))}


def lefts(value, count, dim):
    parts = bf16_parts(value, count)
    return jnp.concatenate([parts[a] for a, _ in PAIRS[count]], axis=dim)


def rights(value, count):
    parts = bf16_parts(value, count)
    return jnp.concatenate([parts[b] for _, b in PAIRS[count]], axis=0)


def products_kernel(tile_ref, left_ref, right_ref, gram_ref, out_ref):
    @pl.when(pl.program_id(0) == 0)
    def _():
        gram_ref[...] = jnp.zeros(gram_ref.shape, jnp.float32)
        out_ref[...] = jnp.zeros(out_ref.shape, jnp.float32)

    panel = jnp.concatenate([left_ref[...], right_ref[...]], axis=1)
    gram_ref[...] += dot(lefts(panel, 3, 0), rights(panel, 3), 0, 0)
    out_ref[...] += dot(lefts(tile_ref[...], 2, 0), rights(panel, 2), 0, 0)


def products(tile, left, right):
    rows_dev, cols_dev = tile.shape
    lines = LINES
    return pl.pallas_call(
        products_kernel,
        out_shape=(
            jax.ShapeDtypeStruct((B, B), jnp.float32),
            jax.ShapeDtypeStruct((cols_dev, B), jnp.float32),
        ),
        grid=(rows_dev // lines,),
        in_specs=[
            pl.BlockSpec((lines, cols_dev), lambda k: (k, 0)),
            pl.BlockSpec((lines, B // 2), lambda k: (k, 0)),
            pl.BlockSpec((lines, B // 2), lambda k: (k, 0)),
        ],
        out_specs=(
            pl.BlockSpec((B, B), lambda k: (0, 0)),
            pl.BlockSpec((cols_dev, B), lambda k: (0, 0)),
        ),
        cost_estimate=pl.CostEstimate(
            flops=6 * rows_dev * (cols_dev + 2 * B) * B,
            bytes_accessed=4 * rows_dev * (cols_dev + B),
            transcendentals=0,
        ),
        interpret=INTERPRET,
        name="products",
    )(tile, left, right)


def update_kernel(
    at_ref, tile_ref, pl_ref, pr_ref, ul_ref, ur_ref, f_ref, w_ref, tv_ref, r_ref, rt_ref, out_ref, factors
):
    row_at, col_at = at_ref[0], at_ref[1]
    step = pl.program_id(0)
    six = 6 * B

    @pl.when(step == 0)
    def _():
        factors[:six, :] = rights(f_ref[...], 3)
        factors[six:, :] = rights(tv_ref[...], 2)

    panel = jnp.concatenate([pl_ref[...], pr_ref[...]], axis=1)
    u_mat = jnp.concatenate([ul_ref[...], ur_ref[...]], axis=1)
    both = jnp.concatenate([lefts(panel, 3, 1), lefts(u_mat, 2, 1)], axis=1)
    out_ref[...] = tile_ref[...] - dot(both, factors[...], 1, 0)

    top = (row_at == 0) & (step == 0)

    @pl.when(top)
    def _():
        out_ref[B : 2 * B, :] = out_ref[B : 2 * B, :] + w_ref[...]

    @pl.when((col_at == 0) & jnp.logical_not(top))
    def _():
        out_ref[:, :B] = jnp.zeros((LINES, B), jnp.float32)

    @pl.when((col_at == 0) & top)
    def _():
        out_ref[B : 2 * B, :B] = r_ref[...]
        out_ref[2 * B :, :B] = jnp.zeros((LINES - 2 * B, B), jnp.float32)
        out_ref[:B, B:] = rt_ref[:, : B // 2]

    @pl.when((col_at == 1) & top)
    def _():
        out_ref[:B, : B // 2] = rt_ref[:, B // 2 :]
        out_ref[:B, B // 2 :] = jnp.zeros((B, B), jnp.float32)

    @pl.when((col_at >= 2) & top)
    def _():
        out_ref[:B, :] = jnp.zeros((B, out_ref.shape[1]), jnp.float32)


def updated(at, tile, panel, u_mat, small, upper):
    rows_dev, cols_dev = tile.shape

    def whole(shape):
        return pl.BlockSpec(shape, lambda k, at: (0, 0))

    def lines(width):
        return pl.BlockSpec((LINES, width), lambda k, at: (k, 0))

    return pl.pallas_call(
        update_kernel,
        out_shape=jax.ShapeDtypeStruct(tile.shape, jnp.float32),
        grid_spec=pltpu.PrefetchScalarGridSpec(
            num_scalar_prefetch=1,
            grid=(rows_dev // LINES,),
            in_specs=[lines(cols_dev)]
            + [lines(B // 2)] * 4
            + [whole((B, cols_dev))] * 3
            + [whole((B, B))] * 2,
            out_specs=lines(cols_dev),
            scratch_shapes=[pltpu.VMEM((9 * B, cols_dev), jnp.bfloat16)],
        ),
        cost_estimate=pl.CostEstimate(
            flops=9 * 2 * rows_dev * cols_dev * B,
            bytes_accessed=4 * rows_dev * (2 * cols_dev + 2 * B),
            transcendentals=0,
        ),
        interpret=INTERPRET,
        name="update",
    )(at, tile, *panel, *u_mat, *small, upper, upper.T)


def per_device(tile):
    _, cols_dev = tile.shape
    row_at = lax.axis_index(ROW)
    col_at = lax.axis_index(COL)
    global_cols = col_at * cols_dev + jnp.arange(cols_dev, dtype=jnp.int32)
    band = jnp.arange(B, dtype=jnp.int32)
    zero = jnp.float32(0.0)

    place = (
        lax.axis_index("c") * 16 + lax.axis_index("y") * 4 + lax.axis_index("zl")
    )
    at = jnp.stack([row_at, col_at]).astype(jnp.int32)

    strip = jnp.where((global_cols >= B)[:, None], tile[:B, :].T, zero)
    panel_part = spread_strip(strip.reshape(8, -1, B))
    panel = plane_gather(panel_part)

    gram, product = products(tile, *panel)
    gram_slice = lax.dynamic_slice_in_dim(gram, place * 8, 8, 0)
    lead_slice = jnp.concatenate(
        [lax.dynamic_slice_in_dim(half, B + place * 8, 8, 0) for half in panel], axis=1
    )
    lead_slice = jnp.where(row_at == 0, lead_slice, zero)
    message = jnp.concatenate([gram_slice, lead_slice], axis=0)
    message = jnp.concatenate(
        [product.reshape(8, -1, B), jnp.broadcast_to(message[None], (8, 16, B))], axis=1
    )
    message = lax.all_to_all(message, ROW, 0, 0, tiled=True)
    message = message.sum(axis=0)
    product_part, message = message[:-16], message[-16:]
    message = from_everyone(from_everyone(message, ("y", "zl")), "c")
    message = message.reshape(32, 2, 8, B)
    gram = message[:, 0].reshape(B, B)
    lead = message[:, 1].reshape(B, B)

    edge = tile[B : 2 * B, :].T.reshape(8, -1, B)
    edge, panel_part, gram = lax.optimization_barrier((edge, panel_part, gram))
    edge = lax.all_to_all(edge, ROW, 0, 0, tiled=True)
    edge = edge.reshape(8, -1, B)[0]
    panel_there = lax.ppermute(panel_part, ALL, TO_ROWS)
    upper, inverse = chol(gram)

    part = panel_there.shape[0]
    both = contract(jnp.concatenate([panel_there, product_part], axis=0), inverse, 1, 1)
    part_rows = col_at * cols_dev + row_at * part + jnp.arange(part, dtype=jnp.int32)
    unit_part = (part_rows[:, None] - B == band[None, :]).astype(jnp.float32)
    u_part = both[part:] - edge
    u_there = lax.ppermute(u_part, ALL, TO_PLANE)
    both_j = row_gather(jnp.concatenate([both[:part] - unit_part, u_part], axis=1))
    t_mat = t_inverse(lead, inverse)
    reflector_j, u_j = both_j[:, :B], both_j[:, B:]

    core_part = contract(reflector_j, u_j, 0, 0).reshape(32, 8, B)
    u_there, core_part = lax.optimization_barrier((u_there, core_part))
    core_part = lax.all_to_all(core_part, COL, 0, 0, tiled=True)
    core_part = core_part.reshape(32, 8, B).sum(axis=0)
    u_left, u_right, core_part = plane_gather(u_there, core_part)
    core_sum = from_everyone(core_part, COL).reshape(B, B)
    middle = contract(contract(t_mat, core_sum, 1, 0), t_mat, 1, 1)

    t_reflector_trans = contract(t_mat, reflector_j, 0, 1)
    w_trans = contract(t_mat, u_j, 1, 1) - contract(middle, reflector_j, 1, 1)
    first_trans = contract(inverse, w_trans, 0, 0)
    return updated(
        at,
        tile,
        panel,
        (u_left, u_right),
        (first_trans, w_trans, t_reflector_trans),
        upper * jnp.float32(1.0 / math.sqrt(N)),
    )


def solution(mesh):
    split = Mesh(mesh.devices.reshape(4, 2, 4, 4, 2), ALL)
    return jax.shard_map(
        per_device,
        mesh=split,
        in_specs=(P(ROW, COL),),
        out_specs=P(ROW, COL),
        check_vma=False,
    )
```
